256 devices in a mesh: obs: 64 (over z, y, core), rep: 4 (over x).
Axes of the slice: x: 4, y: 4, z: 8, core: 2. Of those that a mesh axis runs over, the one named last changes fastest.
Arguments:
- jacobians: float32 [18, 8388608], P(None, ('obs', 'rep')), may hold values from -3 to 3
- residuals: float32 [2, 8388608], P(None, ('obs', 'rep')), may hold values from -6 to 6
- camera_local: int32 [8388608], P(('obs', 'rep')), may hold values from 0 to 1023
- bucket_counts: int32 [256, 64], P(('obs', 'rep')), may hold values from 1 to 512, as said below
- camera_map: int32 [65536], replicated, may hold values from 0 to 65535, each once
Outputs:
- gradient: float32 [9, 65536], replicated
- camera_blocks: float32 [81, 65536], P(None, 'obs')
The draws below stay inside these ranges and needn't reach their ends.
Inputs may be any that keep to these rules, and one draw needn't show every extreme that they name: bucket_counts[s, d] counts the leading live slots of bucket d of source block s; exactly one destination d has all 512 slots live from every source block, and every other bucket has at most 256 live slots. A slot in bucket d names camera slot d * 1024 + camera_local. `camera_map`: each camera id appears once.
All inputs are finite; a program needn't handle non-finite values.
Results may differ from the reference program's by a relative error of at most 0.0003.
Values sent between devices are 32-bit elements; how exact they have to be, the bound alone decides.
A program may use at most 192 MiB of HBM per device.

```python
import math
import jax
import jax.numpy as jnp
import numpy as np
from jax import lax

CAM_DEV = 1024
CAP = 512
CAM = 65536
SLOTS = 8388608
N_OBS = 64
N_REP = 4


def draw_bucket_counts(key, part):
    key_hot = jax.random.fold_in(key, 11)
    key_full = jax.random.fold_in(key, 12)
    key_base = jax.random.fold_in(key, 13)
    hotness = jax.random.randint(key_hot, (N_OBS,), 1, 4)
    full_column = jax.random.randint(key_full, (), 0, N_OBS)
    baseline = jax.random.randint(key_base, (N_OBS * N_REP, N_OBS), CAP // 4, CAP // 2 + 1)
    counts = jnp.minimum(CAP // 2, baseline * hotness[None, :] // 2)
    counts = jnp.maximum(counts, 1)
    column_ids = jnp.arange(N_OBS, dtype=jnp.int32)
    counts = jnp.where(column_ids[None, :] == full_column, CAP, counts)
    return counts.astype(jnp.int32)


def set_ends(drawn, rng, low, largest):
    index_at = [jax.random.randint(jax.random.fold_in(rng, axis), (), 0, length) for axis, length in enumerate(drawn.shape)]
    widest = drawn.shape.index(max(drawn.shape))
    neighbour = index_at[:widest] + [(index_at[widest] + 1) % drawn.shape[widest]] + index_at[widest + 1:]
    return drawn.at[tuple(index_at)].set(low).at[tuple(neighbour)].set(largest)


def block_scale(rng, dims, pieces, smallest, high):
    level, own = 1.0, jax.random.fold_in(rng, 6)
    for dim, shards_of in pieces:
        heights = jnp.exp(jax.random.uniform(jax.random.fold_in(own, dim), (shards_of,), jnp.float32, smallest / len(pieces), high / len(pieces)))
        level = level * jnp.repeat(heights, dims[dim] // shards_of).reshape([-1 if axis == dim else 1 for axis in range(len(dims))])
    return level


def rank_bounds(amount, skew):
    loads = [(1 << 20) // math.isqrt(grade ** skew) + 1 for grade in range(1, amount + 1)]
    scale = 1 + sum(loads) // (1 << 30)
    return np.cumsum(np.array([max(1, weight // scale) for weight in loads]))


def ranked_ids(key, dims, count, lean):
    grid = rank_bounds(count, lean)
    ticket = jax.random.randint(jax.random.fold_in(key, 1), dims, 0, int(grid[count - 1]))
    grade = jnp.searchsorted(jnp.asarray(grid, jnp.int32), ticket, side="right")
    return jax.random.permutation(jax.random.fold_in(key, 2), count)[grade].astype(jnp.int32)


def normal_values(rng, shape, width, most, shards=(), kind=jnp.bfloat16):
    level = block_scale(rng, shape, shards, -0.22, 0.18) if shards else 1.0
    values = jax.random.normal(rng, shape, jnp.float32) * width * level
    return jnp.minimum(jnp.maximum(values, -most), most).astype(kind)


def setup_inputs(seed: int = 0) -> dict:
    key_of = jax.random.split(jax.random.key(seed), 6)
    return {
        "jacobians": normal_values(key_of[0], (18, SLOTS), 0.5, 3.0, ((1, 256),), jnp.float32),
        "residuals": normal_values(key_of[1], (2, SLOTS), 1.0, 6.0, ((1, 256),), jnp.float32),
        "camera_local": set_ends(ranked_ids(key_of[2], (SLOTS,), CAM_DEV, 1), jax.random.fold_in(key_of[2], 3), 0, CAM_DEV - 1).astype(jnp.int32),
        "bucket_counts": draw_bucket_counts(jax.random.fold_in(key_of[5], 71), 0),
        "camera_map": jax.random.permutation(key_of[4], CAM).astype(jnp.int32),
    }


def observation_terms(jacobs, resids):
    leading_row = jacobs[0:9]
    trailing_row = jacobs[9:18]
    gradient_terms = leading_row * resids[0:1] + trailing_row * resids[1:2]
    block_terms = leading_row[:, None] * leading_row[None, :] + trailing_row[:, None] * trailing_row[None, :]
    block_terms = block_terms.reshape((81,) + leading_row.shape[1:])
    return jnp.concatenate([gradient_terms, block_terms], axis=0)


def reference(jacobians, residuals, camera_local, bucket_counts, camera_map):
    sources = N_OBS * N_REP
    columns = N_OBS * CAP
    jac_blocks = jnp.moveaxis(jacobians.reshape(18, sources, columns), 1, 0)
    res_blocks = jnp.moveaxis(residuals.reshape(2, sources, columns), 1, 0)
    cam_blocks = camera_local.reshape(sources, columns)
    position = jnp.arange(columns, dtype=jnp.int32)
    target = position // CAP
    within = position % CAP

    def accumulate(summed, inputs):
        jac_here, res_here, cam_here, count_here = inputs
        live_mask = (within < count_here[target]).astype(jnp.float32)
        obs_terms = observation_terms(jac_here * live_mask, res_here * live_mask)
        segment = (target * CAM_DEV + cam_here).astype(jnp.int32)
        return summed + jax.ops.segment_sum(obs_terms.T, segment, num_segments=CAM), None

    summed, unused = lax.scan(accumulate, jnp.zeros((CAM, 90), jnp.float32), (jac_blocks, res_blocks, cam_blocks, bucket_counts))
    slot_gradient = summed[:, :9].T
    camera_blocks = summed[:, 9:].T
    gradient = jnp.zeros((9, CAM), jnp.float32).at[:, camera_map].set(slot_gradient)
    return gradient, camera_blocks
```

```python
import functools

import jax
import jax.numpy as jnp
from jax import lax
from jax.experimental import pallas as pl
from jax.experimental.pallas import tpu as pltpu
from jax.sharding import PartitionSpec as P

CAM_DEV = 1024
MESH = pl.DeviceIdType.MESH
F32 = jnp.float32
BF16 = jnp.bfloat16
VMEM = pltpu.VMEM
ROWS = 56
HEAD = 16
KEPT = 48
LOW = 256
LIVE = 256
NZ, NY, NX = 8, 4, 4
WINDOWS = (20, 34, 48)
DIMS = (((1,), (1,)), ((), ()))


def split(value):
    high = value.astype(BF16).astype(F32)
    return high, value - high


def one_hot_of(low, wide):
    shape = (wide, low.shape[1])
    rows = lax.broadcasted_iota(jnp.int32, shape, 0).astype(F32).astype(BF16)
    there = jnp.broadcast_to(low.astype(F32), shape).astype(BF16)
    return jnp.where(there == rows, jnp.ones(shape, BF16), jnp.zeros(shape, BF16))


def turn(value, j):
    return jnp.concatenate([value[j:8], value[0:j]], axis=0)


def block_row(k, l):
    k, l = min(k, l), max(k, l)
    if l == 8:
        return 12 if k == 8 else 48 + k
    j = l - k
    if j < 4:
        return 16 + 8 * j + k
    if j == 4:
        return 8 + k
    return 16 + 8 * (8 - j) + l


def add_block(block, acc):
    lead, trail = block[0:8], block[9:17]
    lead8, trail8, res0, res1 = block[8:9], block[17:18], block[18:19], block[19:20]
    ids = block[20:21].astype(jnp.int32)
    place = lax.broadcasted_iota(jnp.int32, lead.shape, 0)

    def mixed(rows, ninth, res):
        left = jnp.where(place < 4, rows, ninth)
        right = jnp.where(place < 4, turn(rows, 4), jnp.where(place == 4, ninth, res))
        return left * right

    groups = [lead * res0 + trail * res1, mixed(lead, lead8, res0) + mixed(trail, trail8, res1)]
    groups.append(lead * lead + trail * trail)
    for j in range(1, 4):
        groups.append(lead * turn(lead, j) + trail * turn(trail, j))
    groups.append(lead * lead8 + trail * trail8)
    high, low = split(jnp.concatenate(groups, axis=0))
    both = jnp.concatenate([high, low], axis=0).astype(BF16)
    pieces, _, width = acc.shape
    up = jnp.where(ids < 0, -1, ids // width)
    one_hot = one_hot_of(ids - up * width, width)
    up = jnp.broadcast_to(up.astype(F32), both.shape).astype(BF16)
    zero = jnp.zeros_like(both)
    lhs = jnp.concatenate([jnp.where(up == jnp.asarray(h, BF16), both, zero) for h in range(pieces)], axis=0)
    added = lax.dot_general(lhs, one_hot, DIMS, preferred_element_type=F32)
    for h in range(pieces):
        at = h * 2 * ROWS
        acc[h] += added[at : at + ROWS] + added[at + ROWS : at + 2 * ROWS]


def place_source(block, up, one_hot, acc):
    rows = jnp.concatenate([block[0:8], block[8:16]], axis=1)
    ninth = jnp.concatenate([block[16:17], block[17:18]], axis=1)
    high, low = split(rows)
    top = jnp.concatenate([high, low], axis=0).astype(BF16)
    high9, low9 = split(ninth)
    up16 = jnp.broadcast_to(up.astype(F32), top.shape).astype(BF16)
    none = jnp.zeros_like(top)
    tiles = [jnp.where(up16 == jnp.asarray(h, BF16), top, none) for h in range(16)]
    mask = up == lax.broadcasted_iota(jnp.int32, (16, up.shape[1]), 0)
    tiles.append(jnp.where(mask, high9, 0.0).astype(BF16))
    tiles.append(jnp.where(mask, low9, 0.0).astype(BF16))
    acc[...] += lax.dot_general(jnp.concatenate(tiles, axis=0), one_hot, DIMS, preferred_element_type=F32)


def main_kernel(
    n, m, counts, jac_in, res_in, ids_in, cmap_in, all_out, blocks_out,
    jac, res, ids, cmap, load_sem, packed, moved, part, landed, blocks, gath, ready, spread, shares, got, every,
    over, over_block, full, over_in, over_z, over_zin, over_m, over_yin, over_g,
    x_send, x_recv, a_send, a_recv, b_send, b_recv, g_send, g_recv, r_send, r_recv, z_send, z_recv, m_send, m_recv,
    l_send, l_recv, p_send, p_recv, ox_send, ox_recv, oz_send, oz_recv, oy_send, oy_recv, og_send, og_recv, out_sem, blocks_sem,
):
    me, rep = lax.axis_index("obs"), lax.axis_index("rep")
    z, y, c, x = me // (NY * 2), lax.rem(me // 2, NY), lax.rem(me, 2), rep
    p = jnp.where(c == 0, x, y)
    q = jnp.where(c == 0, y, x)
    cap = jac.shape[1] // n
    width = part.shape[2]

    def at(zz, yy, cc, xx):
        return {"obs": (zz * NY + yy) * 2 + cc, "rep": xx}

    def cross(pp, qq):
        return at(z, jnp.where(c == 0, qq, pp), c, jnp.where(c == 0, pp, qq))

    barrier = pltpu.get_barrier_semaphore()
    for i in range(1, n):
        pl.semaphore_signal(barrier, inc=1, device_id={"obs": lax.rem(me + i, n)}, device_id_type=MESH)
    for i in range(NY):
        for j in range(1, NX):
            peer = at(z, lax.rem(y + i, NY), c, lax.rem(x + j, NX))
            pl.semaphore_signal(barrier, inc=1, device_id=peer, device_id_type=MESH)
    chunks = load_sem.shape[0] - 3
    span = n // chunks
    loads = [pltpu.make_async_copy(s, d, load_sem.at[k]) for k, (s, d) in enumerate(((res_in, res), (ids_in, ids), (cmap_in, cmap)))]
    for k in range(chunks):
        lanes = pl.ds(k * span * cap, span * cap)
        loads.append(pltpu.make_async_copy(jac_in.at[:, lanes], jac.at[:, lanes], load_sem.at[3 + k]))
    for load in loads:
        load.start()
    part[...] = jnp.zeros_like(part)
    over[...] = jnp.zeros_like(over)
    spread[...] = jnp.zeros_like(spread)
    for load in loads[0:3]:
        load.wait()
    place = lax.broadcasted_iota(jnp.int32, (1, LIVE), 1)

    def pack(d, carry):
        lanes = pl.ds(pl.multiple_of(d * cap, cap), LIVE)
        rest = pl.ds(pl.multiple_of(d * cap + LIVE, LIVE), LIVE)
        packed[d, 0:18, :] = jac[:, lanes]
        packed[d, 18:20, :] = res[:, lanes]
        packed[d, 20:21, :] = jnp.where(place < counts[0, d], ids[:, lanes], -1).astype(F32)
        count = jnp.full((18, LIVE), counts[0, d], jnp.int32)
        late = jnp.where(place + LIVE < counts[0, d], ids[:, rest], -1).astype(F32)
        found = (jac[:, rest], res[:, rest], late, jnp.full((8, LIVE), d, jnp.int32))
        return tuple(jnp.where(count[0 : new.shape[0]] > LIVE, new, old) for new, old in zip(found, carry))

    kept = (jnp.zeros((18, LIVE), F32), jnp.zeros((2, LIVE), F32), jnp.full((1, LIVE), -1, F32), jnp.zeros((8, LIVE), jnp.int32))
    for k in range(chunks):
        loads[3 + k].wait()
        kept = lax.fori_loop(k * span, (k + 1) * span, pack, kept, unroll=4)
    over_block[0:18, :] = kept[0]
    over_block[18:20, :] = kept[1]
    over_block[20:21, :] = kept[2]
    full[...] = kept[3]
    add_block(over_block[...], over)
    pl.semaphore_wait(barrier, n - 1 + NY * (NX - 1))

    def remote(src, dst, s, r, peer):
        return pltpu.make_async_remote_copy(
            src_ref=src, dst_ref=dst, send_sem=s, recv_sem=r, device_id=peer, device_id_type=MESH
        )

    sent = []

    def send(*args):
        copy = remote(*args)
        copy.start()
        sent.append(copy)
        return copy

    def handing(i):
        peer = lax.rem(me + i, n)
        return remote(packed.at[peer], moved.at[i], x_send.at[i], x_recv.at[i], {"obs": peer})

    def start(i, carry):
        handing(i).start()
        return carry

    def take(i, carry):
        handing(i).wait_recv()
        add_block(moved[i], part)
        return carry

    def drain(i, carry):
        handing(i).wait_send()
        return carry

    over_x = []
    for i in (1, 3, 2):
        peer = lax.rem(rep + i, m)
        over_x.append(send(over.at[peer], over_in.at[i], ox_send.at[i], ox_recv.at[i], {"rep": peer}))
    lax.fori_loop(1, WINDOWS[0], start, 0)
    add_block(packed[me], part)

    def prepare(a, carry):
        owner = (a // 2 * NY + y) * 2 + lax.rem(a, 2)
        here = cmap[:, pl.ds(pl.multiple_of(owner * CAM_DEV + rep * width, width), width)]
        ready[a] = one_hot_of(lax.rem(here, LOW), LOW)
        return carry

    lax.fori_loop(0, 16, prepare, 0)
    for copy in over_x:
        copy.wait_recv()
    mine = over[rep] + over_in[1] + over_in[2] + over_in[3]
    for g in range(7):
        over_z[g] = mine[g * 8 : g * 8 + 8]
    over_z[7] = jnp.zeros_like(over_z[7])
    over_zs = []
    for i in range(1, NZ):
        zz = lax.rem(z + i, NZ)
        over_zs.append(send(over_z.at[zz], over_zin.at[i], oz_send.at[i], oz_recv.at[i], at(zz, y, c, x)))
    lax.fori_loop(WINDOWS[0], WINDOWS[1], start, 0)
    lax.fori_loop(1, 17, take, 0)
    for copy in over_zs:
        copy.wait_recv()
    mine = over_z[z]
    for i in range(1, NZ):
        mine = mine + over_zin[i]
    over_m[...] = mine
    over_ys = []
    e = y * 2 + c
    for i in range(1, 8):
        ee = lax.rem(e + i, 8)
        over_ys.append(send(over_m, over_yin.at[i], oy_send.at[i], oy_recv.at[i], at(z, ee // 2, lax.rem(ee, 2), x)))
    lax.fori_loop(WINDOWS[1], WINDOWS[2], start, 0)
    lax.fori_loop(17, 33, take, 0)
    for copy in over_ys:
        copy.wait_recv()
    mine = over_m[...]
    for i in range(1, 8):
        mine = mine + over_yin[i]
    over_g[z] = mine
    over_gs = []
    for i in range(1, NZ):
        over_gs.append(send(over_g.at[z], over_g.at[z], og_send.at[i], og_recv.at[i], at(lax.rem(z + i, NZ), y, c, x)))
    lax.fori_loop(WINDOWS[2], n, start, 0)
    lax.fori_loop(33, n, take, 0)

    first, second = [], []
    for half, rows, copies in ((0, pl.ds(0, HEAD), first), (1, pl.ds(HEAD, ROWS - HEAD), second)):
        for i in (1, 3, 2):
            peer = lax.rem(rep + i, m)
            copies.append(
                send(part.at[peer, rows], landed.at[i, rows], a_send.at[half, i], a_recv.at[half, i], {"rep": peer})
            )
    for i in range(1, NZ):
        slot = over_g.at[lax.rem(z + NZ - i, NZ)]
        remote(slot, slot, og_send.at[i], og_recv.at[i], at(lax.rem(z + i, NZ), y, c, x)).wait_recv()
    owned = full[...] == me
    for copy in first:
        copy.wait_recv()

    def total(g):
        rows = slice(g * 8, g * 8 + 8)
        value = part[rep, rows] + jnp.where(owned, over_g[g], 0.0)
        for i in range(1, m):
            value = value + landed[i, rows]
        return value

    top, mix = total(0), total(1)
    a_me = z * 2 + c
    gath[a_me, 0:8] = top[:, 0:128]
    gath[a_me, 8:16] = top[:, 128:256]
    gath[a_me, 16:17] = mix[5:6, 0:128]
    gath[a_me, 17:18] = mix[5:6, 128:256]
    for i in range(1, 16):
        aa = lax.rem(a_me + i, 16)
        send(gath.at[a_me], gath.at[a_me], g_send.at[i], g_recv.at[i], at(aa // 2, y, lax.rem(aa, 2), x))
    blocks[rep, 0:8] = mix
    for copy in second:
        copy.wait_recv()
    for g in range(2, 7):
        blocks[rep, g * 8 - 8 : g * 8] = total(g)
    wide = []
    for i in (1, 3, 2):
        peer = lax.rem(rep + i, m)
        wide.append(send(blocks.at[rep], blocks.at[rep], b_send.at[i], b_recv.at[i], {"rep": peer}))

    def settle(i, carry):
        a = lax.rem(a_me + 16 - i, 16)
        owner = (a // 2 * NY + y) * 2 + lax.rem(a, 2)
        here = cmap[:, pl.ds(pl.multiple_of(owner * CAM_DEV + rep * width, width), width)]
        place_source(gath[a], here // LOW - a_me * 16, ready[a], spread)
        return carry

    def arrive(i, carry):
        a = lax.rem(a_me + 16 - i, 16)
        aa = lax.rem(a_me + i, 16)
        remote(gath.at[a], gath.at[a], g_send.at[i], g_recv.at[i], at(aa // 2, y, lax.rem(aa, 2), x)).wait_recv()
        return settle(i, carry)

    settle(0, 0)
    lax.fori_loop(1, 16, arrive, 0)
    for u in range(16):
        value = spread[u * 16 : u * 16 + 8, :] + spread[u * 16 + 8 : u * 16 + 16, :]
        shares[u, 0:8] = value[:, 0:128]
        shares[u, 8:16] = value[:, 128:256]
        ninth = spread[256 + u : 257 + u, :] + spread[272 + u : 273 + u, :]
        shares[u, 16:17] = ninth[:, 0:128]
        shares[u, 17:18] = ninth[:, 128:256]
    s_me = p * 4 + q
    reduced = []
    for i in range(1, 16):
        ss = lax.rem(s_me + i, 16)
        reduced.append(send(shares.at[ss], got.at[i], r_send.at[i], r_recv.at[i], cross(ss // 4, lax.rem(ss, 4))))
    for copy in reduced:
        copy.wait_recv()
    value = shares[s_me]
    for i in range(1, 16):
        value = value + got[i]
    every[c, p, q, z] = value
    for i in (4, 3, 5, 2, 6, 1, 7):
        own = every.at[c, p, q, z]
        send(own, own, z_send.at[i], z_recv.at[i], at(lax.rem(z + i, NZ), y, c, x))
    for i in range(1, NZ):
        slot = every.at[c, p, q, lax.rem(z + NZ - i, NZ)]
        remote(slot, slot, z_send.at[i], z_recv.at[i], at(lax.rem(z + i, NZ), y, c, x)).wait_recv()
    outs = []

    def put(cc, pp, qq):
        copy = pltpu.make_async_copy(every.at[cc, pp, qq], all_out.at[cc, pp, qq], out_sem.at[cc, pp, qq])
        copy.start()
        outs.append(copy)

    other = at(z, y, 1 - c, x)

    def back(v, i):
        return lax.rem(v + 4 - i, 4)

    for i in (1, 3, 2):
        group = every.at[c, p, q]
        send(group, group, m_send.at[i], m_recv.at[i], cross(p, lax.rem(q + i, 4)))
    for i in (0, 1, 3, 2):
        group = every.at[c, p, back(q, i)]
        if i:
            remote(group, group, m_send.at[i], m_recv.at[i], cross(p, lax.rem(q + i, 4))).wait_recv()
        for j in (1, 3, 2):
            send(group, group, l_send.at[j, i], l_recv.at[j, i], cross(lax.rem(p + j, 4), q))
        send(group, group, p_send.at[0, i], p_recv.at[0, i], other)
        put(c, p, back(q, i))
    for i in (0, 1, 3, 2):
        for j in (1, 3, 2):
            group = every.at[c, back(p, j), back(q, i)]
            remote(group, group, l_send.at[j, i], l_recv.at[j, i], cross(lax.rem(p + j, 4), q)).wait_recv()
            send(group, group, p_send.at[j, i], p_recv.at[j, i], other)
            put(c, back(p, j), back(q, i))
    for copy in wide:
        copy.wait_recv()
    out_blocks = pltpu.make_async_copy(blocks, blocks_out, blocks_sem.at[0])
    out_blocks.start()
    for j in (0, 1, 3, 2):
        for i in (0, 1, 3, 2):
            group = every.at[1 - c, back(q, j), back(p, i)]
            remote(group, group, p_send.at[j, i], p_recv.at[j, i], other).wait_recv()
            put(1 - c, back(q, j), back(p, i))
    lax.fori_loop(1, n, drain, 0)
    for copy in sent:
        copy.wait_send()
    for copy in outs:
        copy.wait()
    out_blocks.wait()


def write_kernel(all_in, blocks_in, gradient_out, blocks_out, held, blocks, gradient, wide, in_sem, out_sem):
    reads = [pltpu.make_async_copy(all_in.at[:, :, :, k], held.at[:, :, :, k], in_sem.at[k]) for k in range(NZ)]
    reads.append(pltpu.make_async_copy(blocks_in, blocks, in_sem.at[NZ]))
    reads[NZ].start()
    for read in reads[:NZ]:
        read.start()
    step = gradient.shape[1] // NZ
    writes = []

    def write(src, dst, k):
        copy = pltpu.make_async_copy(src, dst, out_sem.at[k])
        copy.start()
        writes.append(copy)

    reads[NZ].wait()
    pieces, _, width = blocks.shape
    for k in range(9):
        for l in range(9):
            row = block_row(k, l) - 8
            for r in range(pieces):
                wide[k * 9 + l : k * 9 + l + 1, r * width : (r + 1) * width] = blocks[r, row : row + 1, :]
    write(wide, blocks_out, NZ)
    for k in range(NZ):
        reads[k].wait()
        for block in range(32):
            c, p, q = block // 16, block // 4 % 4, block % 4
            lanes = k * step + block * LOW
            value = held[c, p, q, k]
            gradient[0:8, lanes : lanes + 128] = value[0:8]
            gradient[0:8, lanes + 128 : lanes + 256] = value[8:16]
            gradient[8:9, lanes : lanes + 128] = value[16:17]
            gradient[8:9, lanes + 128 : lanes + 256] = value[17:18]
        lanes = pl.ds(k * step, step)
        write(gradient.at[:, lanes], gradient_out.at[:, lanes], k)
    for copy in writes:
        copy.wait()


def local(jacobians, residuals, camera_local, bucket_counts, camera_map):
    n, m = lax.axis_size("obs"), lax.axis_size("rep")
    slots = jacobians.shape[1]
    cams = camera_map.shape[0]
    width = CAM_DEV // m
    dma = pltpu.SemaphoreType.DMA
    limit = 60 * 1024 * 1024
    anywhere = pl.BlockSpec(memory_space=pl.ANY)
    hbm = pl.BlockSpec(memory_space=pltpu.HBM)
    gathered, blocks = pl.pallas_call(
        functools.partial(main_kernel, n, m),
        out_shape=(jax.ShapeDtypeStruct((2, 4, 4, NZ, 18, 128), F32), jax.ShapeDtypeStruct((m, KEPT, width), F32)),
        in_specs=[pl.BlockSpec(memory_space=pltpu.SMEM)] + [hbm] * 4,
        out_specs=(hbm, hbm),
        scratch_shapes=[
            VMEM((18, slots), F32),
            VMEM((2, slots), F32),
            VMEM((1, slots), jnp.int32),
            VMEM((1, cams), jnp.int32),
            dma((3 + 4,)),
            VMEM((n, 21, LIVE), F32),
            VMEM((n, 21, LIVE), F32),
            VMEM((m, ROWS, width), F32),
            VMEM((m, ROWS, width), F32),
            VMEM((m, KEPT, width), F32),
            VMEM((16, 18, 128), F32),
            VMEM((16, LOW, width), BF16),
            VMEM((288, LOW), F32),
            VMEM((16, 18, 128), F32),
            VMEM((16, 18, 128), F32),
            VMEM((2, 4, 4, NZ, 18, 128), F32),
            VMEM((m, ROWS, width), F32),
            VMEM((21, LIVE), F32),
            VMEM((8, LIVE), jnp.int32),
            VMEM((m, ROWS, width), F32),
            VMEM((NZ, 8, width), F32),
            VMEM((NZ, 8, width), F32),
            VMEM((8, width), F32),
            VMEM((8, 8, width), F32),
            VMEM((NZ, 8, width), F32),
        ]
        + [dma((n,))] * 2 + [dma((2, m))] * 2 + [dma((m,))] * 2 + [dma((16,))] * 4 + [dma((NZ,))] * 2 + [dma((4,))] * 2
        + [dma((4, 4))] * 4 + [dma((m,))] * 2 + [dma((NZ,))] * 2 + [dma((8,))] * 2 + [dma((NZ,))] * 2
        + [dma((2, 4, 4)), dma((1,))],
        compiler_params=pltpu.CompilerParams(collective_id=0, has_side_effects=True, vmem_limit_bytes=limit),
    )(bucket_counts, jacobians, residuals, camera_local.reshape(1, slots), camera_map.reshape(1, cams))
    shapes = (jax.ShapeDtypeStruct((9, cams), F32), jax.ShapeDtypeStruct((81, CAM_DEV), F32))
    return pl.pallas_call(
        write_kernel,
        out_shape=shapes,
        in_specs=[anywhere] * 2,
        out_specs=(anywhere, anywhere),
        scratch_shapes=[
            VMEM(gathered.shape, F32), VMEM(blocks.shape, F32), VMEM(shapes[0].shape, F32), VMEM(shapes[1].shape, F32),
            dma((NZ + 1,)), dma((NZ + 1,)),
        ],
        compiler_params=pltpu.CompilerParams(vmem_limit_bytes=limit),
    )(gathered, blocks)


def solution(mesh):
    in_specs = (
        P(None, ("obs", "rep")),
        P(None, ("obs", "rep")),
        P(("obs", "rep")),
        P(("obs", "rep"), None),
        P(),
    )
    out_specs = (P(), P(None, "obs"))
    return jax.shard_map(local, mesh=mesh, in_specs=in_specs, out_specs=out_specs, check_vma=False)
```

```python
import functools

import jax
import jax.numpy as jnp
from jax import lax
from jax.experimental import pallas as pl
from jax.experimental.pallas import tpu as pltpu
from jax.sharding import PartitionSpec as P

CAM_DEV = 1024
MESH = pl.DeviceIdType.MESH
F32 = jnp.float32
BF16 = jnp.bfloat16
VMEM = pltpu.VMEM
ROWS = 56
HEAD = 16
KEPT = 48
LOW = 256
LIVE = 256
NZ, NY, NX = 8, 4, 4
AGG = NX * NY * 2
DIMS = (((1,), (1,)), ((), ()))


def split(value):
    high = value.astype(BF16).astype(F32)
    return high, value - high


def one_hot_of(low, wide):
    shape = (wide, low.shape[1])
    rows = lax.broadcasted_iota(jnp.int32, shape, 0).astype(F32).astype(BF16)
    there = jnp.broadcast_to(low.astype(F32), shape).astype(BF16)
    return jnp.where(there == rows, jnp.ones(shape, BF16), jnp.zeros(shape, BF16))


def turn(value, j):
    return jnp.concatenate([value[j:8], value[0:j]], axis=0)


def block_row(k, l):
    k, l = min(k, l), max(k, l)
    if l == 8:
        return 12 if k == 8 else 48 + k
    j = l - k
    if j < 4:
        return 16 + 8 * j + k
    if j == 4:
        return 8 + k
    return 16 + 8 * (8 - j) + l


def add_block(block, acc):
    lead, trail = block[0:8], block[9:17]
    lead8, trail8, res0, res1 = block[8:9], block[17:18], block[18:19], block[19:20]
    ids = block[20:21].astype(jnp.int32)
    place = lax.broadcasted_iota(jnp.int32, lead.shape, 0)

    def mixed(rows, ninth, res):
        left = jnp.where(place < 4, rows, ninth)
        right = jnp.where(place < 4, turn(rows, 4), jnp.where(place == 4, ninth, res))
        return left * right

    groups = [lead * res0 + trail * res1, mixed(lead, lead8, res0) + mixed(trail, trail8, res1)]
    groups.append(lead * lead + trail * trail)
    for j in range(1, 4):
        groups.append(lead * turn(lead, j) + trail * turn(trail, j))
    groups.append(lead * lead8 + trail * trail8)
    high, low = split(jnp.concatenate(groups, axis=0))
    both = jnp.concatenate([high, low], axis=0).astype(BF16)
    pieces, _, width = acc.shape
    up = jnp.where(ids < 0, -1, ids // width)
    one_hot = one_hot_of(ids - up * width, width)
    up = jnp.broadcast_to(up.astype(F32), both.shape).astype(BF16)
    zero = jnp.zeros_like(both)
    lhs = jnp.concatenate([jnp.where(up == jnp.asarray(h, BF16), both, zero) for h in range(pieces)], axis=0)
    added = lax.dot_general(lhs, one_hot, DIMS, preferred_element_type=F32)
    for h in range(pieces):
        at = h * 2 * ROWS
        acc[h, 0:ROWS] += added[at : at + ROWS] + added[at + ROWS : at + 2 * ROWS]


def place_source(block, up, one_hot, acc):
    rows = jnp.concatenate([block[0:8], block[8:16]], axis=1)
    ninth = jnp.concatenate([block[16:17], block[17:18]], axis=1)
    high, low = split(rows)
    top = jnp.concatenate([high, low], axis=0).astype(BF16)
    high9, low9 = split(ninth)
    up16 = jnp.broadcast_to(up.astype(F32), top.shape).astype(BF16)
    none = jnp.zeros_like(top)
    tiles = [jnp.where(up16 == jnp.asarray(h, BF16), top, none) for h in range(16)]
    mask = up == lax.broadcasted_iota(jnp.int32, (16, up.shape[1]), 0)
    tiles.append(jnp.where(mask, high9, 0.0).astype(BF16))
    tiles.append(jnp.where(mask, low9, 0.0).astype(BF16))
    acc[...] += lax.dot_general(jnp.concatenate(tiles, axis=0), one_hot, DIMS, preferred_element_type=F32)


def main_kernel(
    n, m, counts, jac_in, res_in, ids_in, cmap_in, all_out, nine_out, blocks_out,
    jac, res, ids, cmap, load_sem, packed, moved, part, landed, owned_blocks, blocks, gath, ready, spread, shares, got,
    every, nine, over, over_block, full, over_zin, over_m, over_xin, over_n, over_yin, over_g,
    x_send, x_recv, a_send, a_recv, b_send, b_recv, g_send, g_recv, r_send, r_recv, z_send, z_recv, m_send, m_recv,
    l_send, l_recv, p_send, p_recv, oz_send, oz_recv, ox_send, ox_recv, oy_send, oy_recv, og_send, og_recv, out_sem, blocks_sem,
):
    me, rep = lax.axis_index("obs"), lax.axis_index("rep")
    z, y, c, x = me // (NY * 2), lax.rem(me // 2, NY), lax.rem(me, 2), rep
    p = jnp.where(c == 0, x, y)
    q = jnp.where(c == 0, y, x)
    cap = jac.shape[1] // n
    width = part.shape[2]
    e = (x * NY + y) * 2 + c
    half, quarter = z // 4, lax.rem(z, 4)

    def at(zz, yy, cc, xx):
        return {"obs": (zz * NY + yy) * 2 + cc, "rep": xx}

    def cross(pp, qq):
        return at(z, jnp.where(c == 0, qq, pp), c, jnp.where(c == 0, pp, qq))

    chunks = load_sem.shape[0] - 3
    span = n // chunks
    loads = [pltpu.make_async_copy(s, d, load_sem.at[k]) for k, (s, d) in enumerate(((res_in, res), (ids_in, ids), (cmap_in, cmap)))]
    for k in range(chunks):
        lanes = pl.ds(k * span * cap, span * cap)
        loads.append(pltpu.make_async_copy(jac_in.at[:, lanes], jac.at[:, lanes], load_sem.at[3 + k]))
    for load in loads:
        load.start()
    barrier = pltpu.get_barrier_semaphore()

    def plane(i):
        ee = lax.rem(e + i, AGG)
        return at(z, lax.rem(ee // 2, NY), lax.rem(ee, 2), ee // (NY * 2))

    peers = [plane(i) for i in range(1, AGG)]
    for i in range(1, NZ):
        zz = lax.rem(z + i, NZ)
        peers.append(at(zz, y, 1 - c, x))
        for j in range(NX):
            peers.append(at(zz, y, c, lax.rem(x + j, NX)))
    for peer in peers:
        pl.semaphore_signal(barrier, inc=1, device_id=peer, device_id_type=MESH)
    part[...] = jnp.zeros_like(part)
    over[...] = jnp.zeros_like(over)
    spread[...] = jnp.zeros_like(spread)
    for load in loads:
        load.wait()
    place = lax.broadcasted_iota(jnp.int32, (1, LIVE), 1)

    def pack(ee, b):
        d = (ee // 8 * 2 + b) * 8 + lax.rem(ee, 8)
        lanes = pl.ds(pl.multiple_of(d * cap, cap), LIVE)
        packed[ee, b, 0:18, :] = jac[:, lanes]
        packed[ee, b, 18:20, :] = res[:, lanes]
        packed[ee, b, 20:21, :] = jnp.where(place < counts[0, d], ids[:, lanes], -1).astype(F32)

    def scan(d, carry):
        rest = pl.ds(pl.multiple_of(d * cap + LIVE, LIVE), LIVE)
        count = jnp.full((18, LIVE), counts[0, d], jnp.int32)
        late = jnp.where(place + LIVE < counts[0, d], ids[:, rest], -1).astype(F32)
        found = (jac[:, rest], res[:, rest], late, jnp.full((8, LIVE), d, jnp.int32))
        return tuple(jnp.where(count[0 : new.shape[0]] > LIVE, new, old) for new, old in zip(found, carry))

    pl.semaphore_wait(barrier, len(peers))

    def remote(src, dst, s, r, peer):
        return pltpu.make_async_remote_copy(
            src_ref=src, dst_ref=dst, send_sem=s, recv_sem=r, device_id=peer, device_id_type=MESH
        )

    sent = []

    def send(*args):
        copy = remote(*args)
        copy.start()
        sent.append(copy)
        return copy

    def handing(k):
        i = AGG // 2 + (k + 1) // 2 * (1 - 2 * lax.rem(k, 2))
        return remote(packed.at[lax.rem(e + i, AGG)], moved.at[i], x_send.at[i], x_recv.at[i], plane(i))

    def start(k, carry):
        i = AGG // 2 + (k + 1) // 2 * (1 - 2 * lax.rem(k, 2))
        ee = lax.rem(e + i, AGG)
        pack(ee, 0)
        pack(ee, 1)
        handing(k).start()
        return carry

    def take(k, carry):
        i = AGG // 2 + (k + 1) // 2 * (1 - 2 * lax.rem(k, 2))
        handing(k).wait_recv()
        add_block(moved[i, 0], part.at[0:4])
        add_block(moved[i, 1], part.at[4:8])
        return carry

    def drain(k, carry):
        handing(k).wait_send()
        return carry

    far = (4, 3, 5, 2, 6, 1, 7)
    lax.fori_loop(0, 6, start, 0)
    kept = (jnp.zeros((18, LIVE), F32), jnp.zeros((2, LIVE), F32), jnp.full((1, LIVE), -1, F32), jnp.zeros((8, LIVE), jnp.int32))
    kept = lax.fori_loop(0, n, scan, kept, unroll=4)
    over_block[0:18, :] = kept[0]
    over_block[18:20, :] = kept[1]
    over_block[20:21, :] = kept[2]
    full[...] = kept[3]
    add_block(over_block[...], over)

    def over_part(zz):
        return over.at[lax.rem(zz, 4), pl.ds(pl.multiple_of(zz // 4 * 32, 32), 32)]

    over_zs = []
    for i in far:
        zz = lax.rem(z + i, NZ)
        over_zs.append(send(over_part(zz), over_zin.at[i], oz_send.at[i], oz_recv.at[i], at(zz, y, c, x)))
    lax.fori_loop(6, 14, start, 0)
    pack(e, 0)
    pack(e, 1)
    add_block(packed[e, 0], part.at[0:4])
    add_block(packed[e, 1], part.at[4:8])

    def owner_lanes(a):
        owner = (a // NY * 2 + half) * 8 + lax.rem(a, NY) * 2 + c
        return pl.ds(pl.multiple_of(owner * CAM_DEV + quarter * width, width), width)

    def prepare(a, carry):
        ready[a] = one_hot_of(lax.rem(cmap[:, owner_lanes(a)], LOW), LOW)
        return carry

    lax.fori_loop(0, 16, prepare, 0)
    lax.fori_loop(0, 8, take, 0)
    lax.fori_loop(14, 20, start, 0)
    lax.fori_loop(8, 14, take, 0)
    for copy in over_zs:
        copy.wait_recv()
    mine = over_part(z)[...]
    for i in range(1, NZ):
        mine = mine + over_zin[i]
    over_m[...] = mine
    over_xs = []
    for i in (1, 3, 2):
        over_xs.append(send(over_m, over_xin.at[i], ox_send.at[i], ox_recv.at[i], at(z, y, c, lax.rem(x + i, NX))))
    lax.fori_loop(20, 26, start, 0)
    lax.fori_loop(14, 20, take, 0)
    for copy in over_xs:
        copy.wait_recv()
    over_n[...] = over_m[...] + over_xin[1] + over_xin[2] + over_xin[3]
    over_ys = []
    f = y * 2 + c
    for i in (4, 3, 5, 2, 6, 1, 7):
        ff = lax.rem(f + i, 8)
        over_ys.append(send(over_n, over_yin.at[i], oy_send.at[i], oy_recv.at[i], at(z, ff // 2, lax.rem(ff, 2), x)))
    lax.fori_loop(26, AGG - 1, start, 0)
    lax.fori_loop(20, AGG - 1, take, 0)
    first, second = [], []
    for kind, rows, copies in ((0, pl.ds(0, HEAD), first), (1, pl.ds(HEAD, ROWS - HEAD), second)):
        if kind:
            for copy in over_ys:
                copy.wait_recv()
            mine = over_n[...]
            for i in range(1, 8):
                mine = mine + over_yin[i]
            over_g[half] = mine
            send(over_g.at[half], over_g.at[half], og_send.at[0], og_recv.at[0], at(lax.rem(z + 4, NZ), y, c, x))
        for i in far:
            zz = lax.rem(z + i, NZ)
            copies.append(
                send(part.at[zz, rows], landed.at[i, rows], a_send.at[kind, i], a_recv.at[kind, i], at(zz, y, c, x))
            )
    other_half = over_g.at[1 - half]
    remote(other_half, other_half, og_send.at[0], og_recv.at[0], at(lax.rem(z + 4, NZ), y, c, x)).wait_recv()
    bucket = (x * 2 + half) * 8 + y * 2 + c
    owned = full[...] == bucket
    for copy in first:
        copy.wait_recv()

    def total(g):
        rows = slice(g * 8, g * 8 + 8)
        value = part[z, rows] + jnp.where(owned, over_g[g // 4, g % 4 * 8 : g % 4 * 8 + 8], 0.0)
        for i in range(1, NZ):
            value = value + landed[i, rows]
        return value

    top, mix = total(0), total(1)
    a_me = x * NY + y
    gath[a_me, 0:8] = top[:, 0:128]
    gath[a_me, 8:16] = top[:, 128:256]
    gath[a_me, 16:17] = mix[5:6, 0:128]
    gath[a_me, 17:18] = mix[5:6, 128:256]
    def gathering(i):
        a, aa = lax.rem(a_me + 16 - i, 16), lax.rem(a_me + i, 16)
        return gath.at[a], at(z, lax.rem(aa, NY), c, aa // NY)

    for i in (8, 7, 9, 6, 10, 5, 11, 4, 12, 3, 13, 2, 14, 1, 15):
        send(gath.at[a_me], gath.at[a_me], g_send.at[i], g_recv.at[i], gathering(i)[1])
    owned_blocks[0:8] = mix
    for copy in second:
        copy.wait_recv()
    for g in range(2, 7):
        owned_blocks[g * 8 - 8 : g * 8] = total(g)
    home = x * 2 + half
    for j in range(1, NX):
        peer = at(home, y, c, lax.rem(x + j, NX))
        send(owned_blocks, blocks.at[quarter], b_send.at[j], b_recv.at[quarter], peer)

    def to_home():
        return remote(owned_blocks, blocks.at[quarter], b_send.at[0], b_recv.at[quarter], at(home, y, c, x))

    @pl.when(home != z)
    def _():
        to_home().start()

    @pl.when(home == z)
    def _():
        blocks[quarter] = owned_blocks[...]

    def settle(i, carry):
        a = lax.rem(a_me + 16 - i, 16)
        place_source(gath[a], cmap[:, owner_lanes(a)] // LOW - a_me * 16, ready[a], spread)
        return carry

    def arrive(i, carry):
        slot, peer = gathering(i)
        remote(slot, slot, g_send.at[i], g_recv.at[i], peer).wait_recv()
        return settle(i, carry)

    settle(0, 0)
    lax.fori_loop(1, 16, arrive, 0)
    for u in range(16):
        value = spread[u * 16 : u * 16 + 8, :] + spread[u * 16 + 8 : u * 16 + 16, :]
        shares[u, 0:8] = value[:, 0:128]
        shares[u, 8:16] = value[:, 128:256]
        ninth = spread[256 + u : 257 + u, :] + spread[272 + u : 273 + u, :]
        shares[u, 16:17] = ninth[:, 0:128]
        shares[u, 17:18] = ninth[:, 128:256]
    s_me = z * 2 + c
    reduced = []
    for i in (8, 7, 9, 6, 10, 5, 11, 4, 12, 3, 13, 2, 14, 1, 15):
        ss = lax.rem(s_me + i, 16)
        reduced.append(send(shares.at[ss], got.at[i], r_send.at[i], r_recv.at[i], at(ss // 2, y, lax.rem(ss, 2), x)))
    for copy in reduced:
        copy.wait_recv()
    value = shares[s_me]
    for i in range(1, 16):
        value = value + got[i]
    every[c, p, q, z] = value[0:16]
    nine[c, p, q, z] = value[16:18]
    held = (every, nine)
    for i in far:
        for v in (0, 1):
            own = held[v].at[c, p, q, z]
            send(own, own, z_send.at[v, i], z_recv.at[v, i], at(lax.rem(z + i, NZ), y, c, x))
    for i in range(1, NZ):
        for v in (0, 1):
            slot = held[v].at[c, p, q, lax.rem(z + NZ - i, NZ)]
            remote(slot, slot, z_send.at[v, i], z_recv.at[v, i], at(lax.rem(z + i, NZ), y, c, x)).wait_recv()
    outs = []

    def put(v, cc, pp, qq):
        target = (all_out, nine_out)[v]
        copy = pltpu.make_async_copy(held[v].at[cc, pp, qq], target.at[cc, pp, qq], out_sem.at[v, cc, pp, qq])
        copy.start()
        outs.append(copy)

    other = at(z, y, 1 - c, x)

    def back(v, i):
        return lax.rem(v + 4 - i, 4)

    for i in (1, 3, 2):
        for v in (0, 1):
            group = held[v].at[c, p, q]
            send(group, group, m_send.at[v, i], m_recv.at[v, i], cross(p, lax.rem(q + i, 4)))
    for i in (0, 1, 3, 2):
        for v in (0, 1):
            group = held[v].at[c, p, back(q, i)]
            if i:
                remote(group, group, m_send.at[v, i], m_recv.at[v, i], cross(p, lax.rem(q + i, 4))).wait_recv()
            for j in (1, 3, 2):
                send(group, group, l_send.at[v, j, i], l_recv.at[v, j, i], cross(lax.rem(p + j, 4), q))
            send(group, group, p_send.at[v, 0, i], p_recv.at[v, 0, i], other)
            put(v, c, p, back(q, i))
    for i in (0, 1, 3, 2):
        for j in (1, 3, 2):
            for v in (0, 1):
                group = held[v].at[c, back(p, j), back(q, i)]
                remote(group, group, l_send.at[v, j, i], l_recv.at[v, j, i], cross(lax.rem(p + j, 4), q)).wait_recv()
                send(group, group, p_send.at[v, j, i], p_recv.at[v, j, i], other)
                put(v, c, back(p, j), back(q, i))
    for k in range(4):
        slot = blocks.at[k]
        source = lax.rem(z, 2) * 4 + k
        mine_here = (x == z // 2) & (source == z)

        @pl.when(jnp.logical_not(mine_here))
        def _():
            remote(slot, slot, b_send.at[0], b_recv.at[k], at(home, y, c, lax.rem(x + 1, NX))).wait_recv()

    @pl.when(home != z)
    def _():
        to_home().wait_send()

    out_blocks = pltpu.make_async_copy(blocks, blocks_out, blocks_sem.at[0])
    out_blocks.start()
    for j in (0, 1, 3, 2):
        for i in (0, 1, 3, 2):
            for v in (0, 1):
                group = held[v].at[1 - c, back(q, j), back(p, i)]
                remote(group, group, p_send.at[v, j, i], p_recv.at[v, j, i], other).wait_recv()
                put(v, 1 - c, back(q, j), back(p, i))
    lax.fori_loop(0, AGG - 1, drain, 0)
    for copy in sent:
        copy.wait_send()
    for copy in outs:
        copy.wait()
    out_blocks.wait()


def write_kernel(all_in, nine_in, blocks_in, gradient_out, blocks_out, held, nine, blocks, gradient, wide, in_sem, out_sem):
    reads = []
    for k in range(NX * NY):
        x, y = k // NY, k % NY
        for v, (src, dst) in enumerate(((all_in, held), (nine_in, nine))):
            for c, (p, q) in enumerate(((x, y), (y, x))):
                reads.append(pltpu.make_async_copy(src.at[c, p, q], dst.at[c, p, q], in_sem.at[k * 4 + v * 2 + c]))
    last = NX * NY
    reads.append(pltpu.make_async_copy(blocks_in, blocks, in_sem.at[last * 4]))
    for read in reads:
        read.start()
    step = gradient.shape[1] // last
    writes = []

    def write(src, dst, k):
        copy = pltpu.make_async_copy(src, dst, out_sem.at[k])
        copy.start()
        writes.append(copy)

    reads[last * 4].wait()
    pieces, _, width = blocks.shape
    for k in range(9):
        for l in range(9):
            row = block_row(k, l) - 8
            for r in range(pieces):
                wide[k * 9 + l : k * 9 + l + 1, r * width : (r + 1) * width] = blocks[r, row : row + 1, :]
    write(wide, blocks_out, last)
    for k in range(last):
        for read in reads[k * 4 : k * 4 + 4]:
            read.wait()
        x, y = k // NY, k % NY
        for block in range(16):
            z, c = block // 2, block % 2
            p, q = (y, x) if c else (x, y)
            lanes = k * step + block * LOW
            gradient[0:8, lanes : lanes + 128] = held[c, p, q, z, 0:8]
            gradient[0:8, lanes + 128 : lanes + 256] = held[c, p, q, z, 8:16]
            gradient[8:9, lanes : lanes + 128] = nine[c, p, q, z, 0:1]
            gradient[8:9, lanes + 128 : lanes + 256] = nine[c, p, q, z, 1:2]
        lanes = pl.ds(k * step, step)
        write(gradient.at[:, lanes], gradient_out.at[:, lanes], k)
    for copy in writes:
        copy.wait()


def local(jacobians, residuals, camera_local, bucket_counts, camera_map):
    n, m = lax.axis_size("obs"), lax.axis_size("rep")
    slots = jacobians.shape[1]
    cams = camera_map.shape[0]
    width = CAM_DEV // m
    dma = pltpu.SemaphoreType.DMA
    limit = 60 * 1024 * 1024
    anywhere = pl.BlockSpec(memory_space=pl.ANY)
    hbm = pl.BlockSpec(memory_space=pltpu.HBM)
    gathered, ninth, blocks = pl.pallas_call(
        functools.partial(main_kernel, n, m),
        out_shape=(
            jax.ShapeDtypeStruct((2, 4, 4, NZ, 16, 128), F32),
            jax.ShapeDtypeStruct((2, 4, 4, NZ, 2, 128), F32),
            jax.ShapeDtypeStruct((m, KEPT, width), F32),
        ),
        in_specs=[pl.BlockSpec(memory_space=pltpu.SMEM)] + [hbm] * 4,
        out_specs=(hbm, hbm, hbm),
        scratch_shapes=[
            VMEM((18, slots), F32),
            VMEM((2, slots), F32),
            VMEM((1, slots), jnp.int32),
            VMEM((1, cams), jnp.int32),
            dma((3 + 4,)),
            VMEM((AGG, 2, 21, LIVE), F32),
            VMEM((AGG, 2, 21, LIVE), F32),
            VMEM((NZ, ROWS, width), F32),
            VMEM((NZ, ROWS, width), F32),
            VMEM((KEPT, width), F32),
            VMEM((m, KEPT, width), F32),
            VMEM((16, 18, 128), F32),
            VMEM((16, LOW, width), BF16),
            VMEM((288, LOW), F32),
            VMEM((16, 18, 128), F32),
            VMEM((16, 18, 128), F32),
            VMEM((2, 4, 4, NZ, 16, 128), F32),
            VMEM((2, 4, 4, NZ, 2, 128), F32),
            VMEM((m, 64, width), F32),
            VMEM((21, LIVE), F32),
            VMEM((8, LIVE), jnp.int32),
            VMEM((NZ, 32, width), F32),
            VMEM((32, width), F32),
            VMEM((NX, 32, width), F32),
            VMEM((32, width), F32),
            VMEM((8, 32, width), F32),
            VMEM((2, 32, width), F32),
        ]
        + [dma((AGG,))] * 2 + [dma((2, NZ))] * 2 + [dma((4,))] * 2 + [dma((16,))] * 4 + [dma((2, NZ))] * 2 + [dma((2, 4))] * 2
        + [dma((2, 4, 4))] * 4 + [dma((NZ,))] * 2 + [dma((NX,))] * 2 + [dma((8,))] * 2 + [dma((1,))] * 2
        + [dma((2, 2, 4, 4)), dma((1,))],
        compiler_params=pltpu.CompilerParams(collective_id=0, has_side_effects=True, vmem_limit_bytes=limit),
    )(bucket_counts, jacobians, residuals, camera_local.reshape(1, slots), camera_map.reshape(1, cams))
    shapes = (jax.ShapeDtypeStruct((9, cams), F32), jax.ShapeDtypeStruct((81, CAM_DEV), F32))
    return pl.pallas_call(
        write_kernel,
        out_shape=shapes,
        in_specs=[anywhere] * 3,
        out_specs=(anywhere, anywhere),
        scratch_shapes=[
            VMEM(gathered.shape, F32), VMEM(ninth.shape, F32), VMEM(blocks.shape, F32), VMEM(shapes[0].shape, F32),
            VMEM(shapes[1].shape, F32), dma((NX * NY * 4 + 1,)), dma((NX * NY + 1,)),
        ],
        compiler_params=pltpu.CompilerParams(vmem_limit_bytes=limit),
    )(gathered, ninth, blocks)


def solution(mesh):
    in_specs = (
        P(None, ("obs", "rep")),
        P(None, ("obs", "rep")),
        P(("obs", "rep")),
        P(("obs", "rep"), None),
        P(),
    )
    out_specs = (P(), P(None, "obs"))
    return jax.shard_map(local, mesh=mesh, in_specs=in_specs, out_specs=out_specs, check_vma=False)
```

```python
import functools

import jax
import jax.numpy as jnp
from jax import lax
from jax.experimental import pallas as pl
from jax.experimental.pallas import tpu as pltpu
from jax.sharding import PartitionSpec as P

CAM_DEV = 1024
MESH = pl.DeviceIdType.MESH
F32 = jnp.float32
BF16 = jnp.bfloat16
VMEM = pltpu.VMEM
ROWS = 56
HEAD = 16
KEPT = 48
LOW = 256
LIVE = 256
NZ, NY, NX = 8, 4, 4
AGG = NX * NY * 2
DIMS = (((1,), (1,)), ((), ()))


def split(value):
    high = value.astype(BF16).astype(F32)
    return high, value - high


def one_hot_of(low, wide):
    shape = (wide, low.shape[1])
    rows = lax.broadcasted_iota(jnp.int32, shape, 0).astype(F32).astype(BF16)
    there = jnp.broadcast_to(low.astype(F32), shape).astype(BF16)
    return jnp.where(there == rows, jnp.ones(shape, BF16), jnp.zeros(shape, BF16))


def turn(value, j):
    return jnp.concatenate([value[j:8], value[0:j]], axis=0)


def block_row(k, l):
    k, l = min(k, l), max(k, l)
    if l == 8:
        return 12 if k == 8 else 48 + k
    j = l - k
    if j < 4:
        return 16 + 8 * j + k
    if j == 4:
        return 8 + k
    return 16 + 8 * (8 - j) + l


def add_block(block, acc):
    lead, trail = block[0:8], block[9:17]
    lead8, trail8, res0, res1 = block[8:9], block[17:18], block[18:19], block[19:20]
    ids = block[20:21].astype(jnp.int32)
    place = lax.broadcasted_iota(jnp.int32, lead.shape, 0)

    def mixed(rows, ninth, res):
        left = jnp.where(place < 4, rows, ninth)
        right = jnp.where(place < 4, turn(rows, 4), jnp.where(place == 4, ninth, res))
        return left * right

    groups = [lead * res0 + trail * res1, mixed(lead, lead8, res0) + mixed(trail, trail8, res1)]
    groups.append(lead * lead + trail * trail)
    for j in range(1, 4):
        groups.append(lead * turn(lead, j) + trail * turn(trail, j))
    groups.append(lead * lead8 + trail * trail8)
    high, low = split(jnp.concatenate(groups, axis=0))
    both = jnp.concatenate([high, low], axis=0).astype(BF16)
    pieces, _, width = acc.shape
    up = jnp.where(ids < 0, -1, ids // width)
    one_hot = one_hot_of(ids - up * width, width)
    up = jnp.broadcast_to(up.astype(F32), both.shape).astype(BF16)
    zero = jnp.zeros_like(both)
    lhs = jnp.concatenate([jnp.where(up == jnp.asarray(h, BF16), both, zero) for h in range(pieces)], axis=0)
    added = lax.dot_general(lhs, one_hot, DIMS, preferred_element_type=F32)
    for h in range(pieces):
        at = h * 2 * ROWS
        acc[h, 0:ROWS] += added[at : at + ROWS] + added[at + ROWS : at + 2 * ROWS]


def place_source(block, up, one_hot, acc):
    rows = jnp.concatenate([block[0:8], block[8:16]], axis=1)
    ninth = jnp.concatenate([block[16:17], block[17:18]], axis=1)
    high, low = split(rows)
    top = jnp.concatenate([high, low], axis=0).astype(BF16)
    high9, low9 = split(ninth)
    up16 = jnp.broadcast_to(up.astype(F32), top.shape).astype(BF16)
    none = jnp.zeros_like(top)
    tiles = [jnp.where(up16 == jnp.asarray(h, BF16), top, none) for h in range(16)]
    mask = up == lax.broadcasted_iota(jnp.int32, (16, up.shape[1]), 0)
    tiles.append(jnp.where(mask, high9, 0.0).astype(BF16))
    tiles.append(jnp.where(mask, low9, 0.0).astype(BF16))
    acc[...] += lax.dot_general(jnp.concatenate(tiles, axis=0), one_hot, DIMS, preferred_element_type=F32)


def main_kernel(
    n, m, counts, jac_in, res_in, ids_in, cmap_in, all_out, nine_out, blocks_out,
    jac, res, ids, cmap, load_sem, packed, moved, part, landed, row_blocks, blocks, gath, ready, spread, shares, got,
    every, nine, over, over_block, full, over_zin, over_s, over_in, over_all,
    x_send, x_recv, a_send, a_recv, b_send, b_recv, h_send, h_recv, g_send, g_recv, r_send, r_recv, z_send, z_recv,
    m_send, m_recv, l_send, l_recv, p_send, p_recv, oz_send, oz_recv, or_send, or_recv, og_send, og_recv, out_sem, blocks_sem,
):
    me, rep = lax.axis_index("obs"), lax.axis_index("rep")
    z, y, c, x = me // (NY * 2), lax.rem(me // 2, NY), lax.rem(me, 2), rep
    p = jnp.where(c == 0, x, y)
    q = jnp.where(c == 0, y, x)
    cap = jac.shape[1] // n
    width = part.shape[2]
    e = (x * NY + y) * 2 + c
    half, quarter = z // 4, lax.rem(z, 4)

    def at(zz, yy, cc, xx):
        return {"obs": (zz * NY + yy) * 2 + cc, "rep": xx}

    def cross(pp, qq):
        return at(z, jnp.where(c == 0, qq, pp), c, jnp.where(c == 0, pp, qq))

    chunks = load_sem.shape[0] - 3
    span = n // chunks
    loads = [pltpu.make_async_copy(s, d, load_sem.at[k]) for k, (s, d) in enumerate(((res_in, res), (ids_in, ids), (cmap_in, cmap)))]
    for k in range(chunks):
        lanes = pl.ds(k * span * cap, span * cap)
        loads.append(pltpu.make_async_copy(jac_in.at[:, lanes], jac.at[:, lanes], load_sem.at[3 + k]))
    for load in loads:
        load.start()
    barrier = pltpu.get_barrier_semaphore()

    def plane(i):
        ee = lax.rem(e + i, AGG)
        return at(z, lax.rem(ee // 2, NY), lax.rem(ee, 2), ee // (NY * 2))

    peers = [plane(i) for i in range(1, AGG)]
    for i in range(1, NZ):
        zz = lax.rem(z + i, NZ)
        peers.append(at(zz, y, c, x))
        peers.append(at(zz, y, 1 - c, x))
    for peer in peers:
        pl.semaphore_signal(barrier, inc=1, device_id=peer, device_id_type=MESH)
    part[...] = jnp.zeros_like(part)
    over[...] = jnp.zeros_like(over)
    spread[...] = jnp.zeros_like(spread)
    for load in loads:
        load.wait()
    place = lax.broadcasted_iota(jnp.int32, (1, LIVE), 1)

    def pack(ee, b):
        d = (ee // 8 * 2 + b) * 8 + lax.rem(ee, 8)
        lanes = pl.ds(pl.multiple_of(d * cap, cap), LIVE)
        packed[ee, b, 0:18, :] = jac[:, lanes]
        packed[ee, b, 18:20, :] = res[:, lanes]
        packed[ee, b, 20:21, :] = jnp.where(place < counts[0, d], ids[:, lanes], -1).astype(F32)

    def scan(d, carry):
        rest = pl.ds(pl.multiple_of(d * cap + LIVE, LIVE), LIVE)
        count = jnp.full((18, LIVE), counts[0, d], jnp.int32)
        late = jnp.where(place + LIVE < counts[0, d], ids[:, rest], -1).astype(F32)
        found = (jac[:, rest], res[:, rest], late, jnp.full((8, LIVE), d, jnp.int32))
        return tuple(jnp.where(count[0 : new.shape[0]] > LIVE, new, old) for new, old in zip(found, carry))

    pl.semaphore_wait(barrier, len(peers))

    def remote(src, dst, s, r, peer):
        return pltpu.make_async_remote_copy(
            src_ref=src, dst_ref=dst, send_sem=s, recv_sem=r, device_id=peer, device_id_type=MESH
        )

    sent = []

    def send(*args):
        copy = remote(*args)
        copy.start()
        sent.append(copy)
        return copy

    def handing(k):
        i = AGG // 2 + (k + 1) // 2 * (1 - 2 * lax.rem(k, 2))
        return remote(packed.at[lax.rem(e + i, AGG)], moved.at[i], x_send.at[i], x_recv.at[i], plane(i))

    def start(k, carry):
        i = AGG // 2 + (k + 1) // 2 * (1 - 2 * lax.rem(k, 2))
        ee = lax.rem(e + i, AGG)
        pack(ee, 0)
        pack(ee, 1)
        handing(k).start()
        return carry

    def take(k, carry):
        i = AGG // 2 + (k + 1) // 2 * (1 - 2 * lax.rem(k, 2))
        handing(k).wait_recv()
        add_block(moved[i, 0], part.at[0:4])
        add_block(moved[i, 1], part.at[4:8])
        return carry

    def drain(k, carry):
        handing(k).wait_send()
        return carry

    far = (4, 3, 5, 2, 6, 1, 7)
    lax.fori_loop(0, 6, start, 0)
    kept = (jnp.zeros((18, LIVE), F32), jnp.zeros((2, LIVE), F32), jnp.full((1, LIVE), -1, F32), jnp.zeros((8, LIVE), jnp.int32))
    kept = lax.fori_loop(0, n, scan, kept, unroll=4)
    over_block[0:18, :] = kept[0]
    over_block[18:20, :] = kept[1]
    over_block[20:21, :] = kept[2]
    full[...] = kept[3]
    add_block(over_block[...], over)

    over_zs = []
    for i in far:
        zz = lax.rem(z + i, NZ)
        over_zs.append(send(over.at[lax.rem(zz, 4)], over_zin.at[i], oz_send.at[i], oz_recv.at[i], at(zz, y, c, x)))
    lax.fori_loop(6, AGG - 1, start, 0)
    pack(e, 0)
    pack(e, 1)
    add_block(packed[e, 0], part.at[0:4])
    add_block(packed[e, 1], part.at[4:8])

    def owner_lanes(a):
        owner = (a // NY * 2 + half) * 8 + lax.rem(a, NY) * 2 + c
        return pl.ds(pl.multiple_of(owner * CAM_DEV + quarter * width, width), width)

    def prepare(a, carry):
        ready[a] = one_hot_of(lax.rem(cmap[:, owner_lanes(a)], LOW), LOW)
        return carry

    lax.fori_loop(0, 16, prepare, 0)
    lax.fori_loop(0, 24, take, 0)
    for copy in over_zs:
        copy.wait_recv()
    mine = over[quarter]
    for i in range(1, NZ):
        mine = mine + over_zin[i]
    for k in range(ROWS // 2):
        over_s[k] = mine[k * 2 : k * 2 + 2]
    for k in range(ROWS // 2, AGG):
        over_s[k] = jnp.zeros_like(over_s[k])

    def scattering(i, carry):
        remote(over_s.at[lax.rem(e + i, AGG)], over_in.at[i], or_send.at[i], or_recv.at[i], plane(i)).start()
        return carry

    def gathering_over(i):
        slot = over_all.at[lax.rem(e + AGG - i, AGG)]
        return remote(slot, slot, og_send.at[i], og_recv.at[i], plane(i))

    def spreading(i, carry):
        slot = over_all.at[e]
        remote(slot, slot, og_send.at[i], og_recv.at[i], plane(i)).start()
        return carry

    def added(i, value):
        remote(over_s.at[i], over_in.at[i], or_send.at[i], or_recv.at[i], plane(i)).wait_recv()
        return value + over_in[i]

    def arrived(i, carry):
        gathering_over(i).wait_recv()
        return carry

    def drain_over(i, carry):
        remote(over_s.at[lax.rem(e + i, AGG)], over_in.at[i], or_send.at[i], or_recv.at[i], plane(i)).wait_send()
        gathering_over(i).wait_send()
        return carry

    lax.fori_loop(1, AGG, scattering, 0)
    lax.fori_loop(24, AGG - 1, take, 0)
    first, second = [], []
    for kind, rows, copies in ((0, pl.ds(0, HEAD), first), (1, pl.ds(HEAD, ROWS - HEAD), second)):
        for i in far:
            zz = lax.rem(z + i, NZ)
            copies.append(
                send(part.at[zz, rows], landed.at[i, rows], a_send.at[kind, i], a_recv.at[kind, i], at(zz, y, c, x))
            )
    over_all[e] = lax.fori_loop(1, AGG, added, over_s[e])
    lax.fori_loop(1, AGG, spreading, 0)
    lax.fori_loop(1, AGG, arrived, 0)
    bucket = (x * 2 + half) * 8 + y * 2 + c
    owned = full[...] == bucket
    for copy in first:
        copy.wait_recv()

    def total(g):
        rows = slice(g * 8, g * 8 + 8)
        value = part[z, rows] + jnp.where(owned, jnp.concatenate([over_all[g * 4 + i] for i in range(4)], axis=0), 0.0)
        for i in range(1, NZ):
            value = value + landed[i, rows]
        return value

    top, mix = total(0), total(1)
    a_me = x * NY + y
    gath[a_me, 0:8] = top[:, 0:128]
    gath[a_me, 8:16] = top[:, 128:256]
    gath[a_me, 16:17] = mix[5:6, 0:128]
    gath[a_me, 17:18] = mix[5:6, 128:256]
    def gathering(i):
        a, aa = lax.rem(a_me + 16 - i, 16), lax.rem(a_me + i, 16)
        return gath.at[a], at(z, lax.rem(aa, NY), c, aa // NY)

    for i in (8, 7, 9, 6, 10, 5, 11, 4, 12, 3, 13, 2, 14, 1, 15):
        send(gath.at[a_me], gath.at[a_me], g_send.at[i], g_recv.at[i], gathering(i)[1])
    row_blocks[x, 0:8] = mix
    for copy in second:
        copy.wait_recv()
    for g in range(2, 7):
        row_blocks[x, g * 8 - 8 : g * 8] = total(g)
    row = []
    for i in (1, 3, 2):
        piece = row_blocks.at[x]
        row.append(send(piece, piece, b_send.at[i], b_recv.at[i], at(z, y, c, lax.rem(x + i, NX))))

    def settle(i, carry):
        a = lax.rem(a_me + 16 - i, 16)
        place_source(gath[a], cmap[:, owner_lanes(a)] // LOW - a_me * 16, ready[a], spread)
        return carry

    def arrive(i, carry):
        slot, peer = gathering(i)
        remote(slot, slot, g_send.at[i], g_recv.at[i], peer).wait_recv()
        return settle(i, carry)

    settle(0, 0)
    lax.fori_loop(1, 16, arrive, 0)
    for u in range(16):
        value = spread[u * 16 : u * 16 + 8, :] + spread[u * 16 + 8 : u * 16 + 16, :]
        shares[u, 0:8] = value[:, 0:128]
        shares[u, 8:16] = value[:, 128:256]
        ninth = spread[256 + u : 257 + u, :] + spread[272 + u : 273 + u, :]
        shares[u, 16:17] = ninth[:, 0:128]
        shares[u, 17:18] = ninth[:, 128:256]
    s_me = z * 2 + c
    reduced = []
    for i in (8, 7, 9, 6, 10, 5, 11, 4, 12, 3, 13, 2, 14, 1, 15):
        ss = lax.rem(s_me + i, 16)
        reduced.append(send(shares.at[ss], got.at[i], r_send.at[i], r_recv.at[i], at(ss // 2, y, lax.rem(ss, 2), x)))
    for copy in reduced:
        copy.wait_recv()
    value = shares[s_me]
    for i in range(1, 16):
        value = value + got[i]
    every[c, p, q, z] = value[0:16]
    nine[c, p, q, z] = value[16:18]
    held = (every, nine)
    for i in far:
        for v in (0, 1):
            own = held[v].at[c, p, q, z]
            send(own, own, z_send.at[v, i], z_recv.at[v, i], at(lax.rem(z + i, NZ), y, c, x))
    for i in range(1, NZ):
        for v in (0, 1):
            slot = held[v].at[c, p, q, lax.rem(z + NZ - i, NZ)]
            remote(slot, slot, z_send.at[v, i], z_recv.at[v, i], at(lax.rem(z + i, NZ), y, c, x)).wait_recv()
    outs = []

    def put(v, cc, pp, qq):
        target = (all_out, nine_out)[v]
        copy = pltpu.make_async_copy(held[v].at[cc, pp, qq], target.at[cc, pp, qq], out_sem.at[v, cc, pp, qq])
        copy.start()
        outs.append(copy)

    other = at(z, y, 1 - c, x)

    def back(v, i):
        return lax.rem(v + 4 - i, 4)

    for i in (1, 3, 2):
        for v in (0, 1):
            group = held[v].at[c, p, q]
            send(group, group, m_send.at[v, i], m_recv.at[v, i], cross(p, lax.rem(q + i, 4)))
    for i in range(1, NX):
        piece = row_blocks.at[lax.rem(x + NX - i, NX)]
        remote(piece, piece, b_send.at[i], b_recv.at[i], at(z, y, c, lax.rem(x + i, NX))).wait_recv()

    def homing(k):
        return remote(row_blocks.at[k], blocks.at[quarter], h_send.at[k], h_recv.at[quarter], at(k * 2 + half, y, c, x))

    for k in range(NX):

        @pl.when(k * 2 + half != z)
        def _():
            homing(k).start()

        @pl.when(k * 2 + half == z)
        def _():
            blocks[quarter] = row_blocks[k]

    for i in (0, 1, 3, 2):
        for v in (0, 1):
            group = held[v].at[c, p, back(q, i)]
            if i:
                remote(group, group, m_send.at[v, i], m_recv.at[v, i], cross(p, lax.rem(q + i, 4))).wait_recv()
            for j in (1, 3, 2):
                send(group, group, l_send.at[v, j, i], l_recv.at[v, j, i], cross(lax.rem(p + j, 4), q))
            send(group, group, p_send.at[v, 0, i], p_recv.at[v, 0, i], other)
            put(v, c, p, back(q, i))
    for i in (0, 1, 3, 2):
        for j in (1, 3, 2):
            for v in (0, 1):
                group = held[v].at[c, back(p, j), back(q, i)]
                remote(group, group, l_send.at[v, j, i], l_recv.at[v, j, i], cross(lax.rem(p + j, 4), q)).wait_recv()
                send(group, group, p_send.at[v, j, i], p_recv.at[v, j, i], other)
                put(v, c, back(p, j), back(q, i))
    for k in range(4):
        slot = blocks.at[k]

        @pl.when(lax.rem(z, 2) * 4 + k != z)
        def _():
            remote(slot, slot, h_send.at[0], h_recv.at[k], at(lax.rem(z + 1, NZ), y, c, x)).wait_recv()

        @pl.when(k * 2 + half != z)
        def _():
            homing(k).wait_send()

    out_blocks = pltpu.make_async_copy(blocks, blocks_out, blocks_sem.at[0])
    out_blocks.start()
    for j in (0, 1, 3, 2):
        for i in (0, 1, 3, 2):
            for v in (0, 1):
                group = held[v].at[1 - c, back(q, j), back(p, i)]
                remote(group, group, p_send.at[v, j, i], p_recv.at[v, j, i], other).wait_recv()
                put(v, 1 - c, back(q, j), back(p, i))
    lax.fori_loop(0, AGG - 1, drain, 0)
    lax.fori_loop(1, AGG, drain_over, 0)
    for copy in sent:
        copy.wait_send()
    for copy in outs:
        copy.wait()
    out_blocks.wait()


def write_kernel(all_in, nine_in, blocks_in, gradient_out, blocks_out, held, nine, blocks, gradient, wide, in_sem, out_sem):
    reads = []
    for k in range(NX):
        for v, (src, dst) in enumerate(((all_in, held), (nine_in, nine))):
            for c, cut in enumerate(((0, k), (1, slice(None), k))):
                reads.append(pltpu.make_async_copy(src.at[cut], dst.at[cut], in_sem.at[k * 4 + v * 2 + c]))
    last = NX
    reads.append(pltpu.make_async_copy(blocks_in, blocks, in_sem.at[last * 4]))
    for read in reads:
        read.start()
    step = gradient.shape[1] // last
    writes = []

    def write(src, dst, k):
        copy = pltpu.make_async_copy(src, dst, out_sem.at[k])
        copy.start()
        writes.append(copy)

    reads[last * 4].wait()
    pieces, _, width = blocks.shape
    for k in range(9):
        for l in range(9):
            row = block_row(k, l) - 8
            for r in range(pieces):
                wide[k * 9 + l : k * 9 + l + 1, r * width : (r + 1) * width] = blocks[r, row : row + 1, :]
    write(wide, blocks_out, last)
    for k in range(last):
        for read in reads[k * 4 : k * 4 + 4]:
            read.wait()
        for block in range(64):
            y, z, c = block // 16, block // 2 % 8, block % 2
            p, q = (y, k) if c else (k, y)
            lanes = k * step + block * LOW
            gradient[0:8, lanes : lanes + 128] = held[c, p, q, z, 0:8]
            gradient[0:8, lanes + 128 : lanes + 256] = held[c, p, q, z, 8:16]
            gradient[8:9, lanes : lanes + 128] = nine[c, p, q, z, 0:1]
            gradient[8:9, lanes + 128 : lanes + 256] = nine[c, p, q, z, 1:2]
        lanes = pl.ds(k * step, step)
        write(gradient.at[:, lanes], gradient_out.at[:, lanes], k)
    for copy in writes:
        copy.wait()


def local(jacobians, residuals, camera_local, bucket_counts, camera_map):
    n, m = lax.axis_size("obs"), lax.axis_size("rep")
    slots = jacobians.shape[1]
    cams = camera_map.shape[0]
    width = CAM_DEV // m
    dma = pltpu.SemaphoreType.DMA
    limit = 60 * 1024 * 1024
    anywhere = pl.BlockSpec(memory_space=pl.ANY)
    hbm = pl.BlockSpec(memory_space=pltpu.HBM)
    gathered, ninth, blocks = pl.pallas_call(
        functools.partial(main_kernel, n, m),
        out_shape=(
            jax.ShapeDtypeStruct((2, 4, 4, NZ, 16, 128), F32),
            jax.ShapeDtypeStruct((2, 4, 4, NZ, 2, 128), F32),
            jax.ShapeDtypeStruct((m, KEPT, width), F32),
        ),
        in_specs=[pl.BlockSpec(memory_space=pltpu.SMEM)] + [hbm] * 4,
        out_specs=(hbm, hbm, hbm),
        scratch_shapes=[
            VMEM((18, slots), F32),
            VMEM((2, slots), F32),
            VMEM((1, slots), jnp.int32),
            VMEM((1, cams), jnp.int32),
            dma((3 + 4,)),
            VMEM((AGG, 2, 21, LIVE), F32),
            VMEM((AGG, 2, 21, LIVE), F32),
            VMEM((NZ, ROWS, width), F32),
            VMEM((NZ, ROWS, width), F32),
            VMEM((NX, KEPT, width), F32),
            VMEM((m, KEPT, width), F32),
            VMEM((16, 18, 128), F32),
            VMEM((16, LOW, width), BF16),
            VMEM((288, LOW), F32),
            VMEM((16, 18, 128), F32),
            VMEM((16, 18, 128), F32),
            VMEM((2, 4, 4, NZ, 16, 128), F32),
            VMEM((2, 4, 4, NZ, 2, 128), F32),
            VMEM((m, ROWS, width), F32),
            VMEM((21, LIVE), F32),
            VMEM((8, LIVE), jnp.int32),
            VMEM((NZ, ROWS, width), F32),
            VMEM((AGG, 2, width), F32),
            VMEM((AGG, 2, width), F32),
            VMEM((AGG, 2, width), F32),
        ]
        + [dma((AGG,))] * 2 + [dma((2, NZ))] * 2 + [dma((4,))] * 4 + [dma((16,))] * 4 + [dma((2, NZ))] * 2 + [dma((2, 4))] * 2
        + [dma((2, 4, 4))] * 4 + [dma((NZ,))] * 2 + [dma((AGG,))] * 4 + [dma((2, 2, 4, 4)), dma((1,))],
        compiler_params=pltpu.CompilerParams(collective_id=0, has_side_effects=True, vmem_limit_bytes=limit),
    )(bucket_counts, jacobians, residuals, camera_local.reshape(1, slots), camera_map.reshape(1, cams))
    shapes = (jax.ShapeDtypeStruct((9, cams), F32), jax.ShapeDtypeStruct((81, CAM_DEV), F32))
    return pl.pallas_call(
        write_kernel,
        out_shape=shapes,
        in_specs=[anywhere] * 3,
        out_specs=(anywhere, anywhere),
        scratch_shapes=[
            VMEM(gathered.shape, F32), VMEM(ninth.shape, F32), VMEM(blocks.shape, F32), VMEM(shapes[0].shape, F32),
            VMEM(shapes[1].shape, F32), dma((NX * 4 + 1,)), dma((NX + 1,)),
        ],
        compiler_params=pltpu.CompilerParams(vmem_limit_bytes=limit),
    )(gathered, ninth, blocks)


def solution(mesh):
    in_specs = (
        P(None, ("obs", "rep")),
        P(None, ("obs", "rep")),
        P(("obs", "rep")),
        P(("obs", "rep"), None),
        P(),
    )
    out_specs = (P(), P(None, "obs"))
    return jax.shard_map(local, mesh=mesh, in_specs=in_specs, out_specs=out_specs, check_vma=False)
```

```python
import functools

import jax
import jax.numpy as jnp
from jax import lax
from jax.experimental import pallas as pl
from jax.experimental.pallas import tpu as pltpu
from jax.sharding import PartitionSpec as P

CAM_DEV = 1024
MESH = pl.DeviceIdType.MESH
F32 = jnp.float32
BF16 = jnp.bfloat16
VMEM = pltpu.VMEM
ROWS = 56
HEAD = 16
KEPT = 48
LOW = 256
LIVE = 256
NZ, NY, NX = 8, 4, 4
AGG = NX * NY * 2
DIMS = (((1,), (1,)), ((), ()))


def split(value):
    high = value.astype(BF16).astype(F32)
    return high, value - high


def one_hot_of(low, wide):
    shape = (wide, low.shape[1])
    rows = lax.broadcasted_iota(jnp.int32, shape, 0).astype(F32).astype(BF16)
    there = jnp.broadcast_to(low.astype(F32), shape).astype(BF16)
    return jnp.where(there == rows, jnp.ones(shape, BF16), jnp.zeros(shape, BF16))


def turn(value, j):
    return jnp.concatenate([value[j:8], value[0:j]], axis=0)


def block_row(k, l):
    k, l = min(k, l), max(k, l)
    if l == 8:
        return 12 if k == 8 else 48 + k
    j = l - k
    if j < 4:
        return 16 + 8 * j + k
    if j == 4:
        return 8 + k
    return 16 + 8 * (8 - j) + l


def add_block(block, acc):
    lead, trail = block[0:8], block[9:17]
    lead8, trail8, res0, res1 = block[8:9], block[17:18], block[18:19], block[19:20]
    ids = block[20:21].astype(jnp.int32)
    place = lax.broadcasted_iota(jnp.int32, lead.shape, 0)

    def mixed(rows, ninth, res):
        left = jnp.where(place < 4, rows, ninth)
        right = jnp.where(place < 4, turn(rows, 4), jnp.where(place == 4, ninth, res))
        return left * right

    groups = [lead * res0 + trail * res1, mixed(lead, lead8, res0) + mixed(trail, trail8, res1)]
    groups.append(lead * lead + trail * trail)
    for j in range(1, 4):
        groups.append(lead * turn(lead, j) + trail * turn(trail, j))
    groups.append(lead * lead8 + trail * trail8)
    high, low = split(jnp.concatenate(groups, axis=0))
    both = jnp.concatenate([high, low], axis=0).astype(BF16)
    pieces, _, width = acc.shape
    up = jnp.where(ids < 0, -1, ids // width)
    one_hot = one_hot_of(ids - up * width, width)
    up = jnp.broadcast_to(up.astype(F32), both.shape).astype(BF16)
    zero = jnp.zeros_like(both)
    lhs = jnp.concatenate([jnp.where(up == jnp.asarray(h, BF16), both, zero) for h in range(pieces)], axis=0)
    added = lax.dot_general(lhs, one_hot, DIMS, preferred_element_type=F32)
    for h in range(pieces):
        at = h * 2 * ROWS
        acc[h, 0:ROWS] += added[at : at + ROWS] + added[at + ROWS : at + 2 * ROWS]


def place_source(block, up, one_hot, acc):
    rows = jnp.concatenate([block[0:8], block[8:16]], axis=1)
    ninth = jnp.concatenate([block[16:17], block[17:18]], axis=1)
    high, low = split(rows)
    top = jnp.concatenate([high, low], axis=0).astype(BF16)
    high9, low9 = split(ninth)
    up16 = jnp.broadcast_to(up.astype(F32), top.shape).astype(BF16)
    none = jnp.zeros_like(top)
    tiles = [jnp.where(up16 == jnp.asarray(h, BF16), top, none) for h in range(16)]
    mask = up == lax.broadcasted_iota(jnp.int32, (16, up.shape[1]), 0)
    tiles.append(jnp.where(mask, high9, 0.0).astype(BF16))
    tiles.append(jnp.where(mask, low9, 0.0).astype(BF16))
    acc[...] += lax.dot_general(jnp.concatenate(tiles, axis=0), one_hot, DIMS, preferred_element_type=F32)


def main_kernel(
    n, m, counts, jac_in, res_in, ids_in, cmap_in, all_out, nine_out, blocks_out,
    jac, res, ids, cmap, load_sem, packed, moved, part, landed, row_blocks, blocks, gath, ready, spread, shares, got,
    every, nine, over, over_block, full, over_zin, over_s, over_in, over_all,
    x_send, x_recv, a_send, a_recv, b_send, b_recv, h_send, h_recv, g_send, g_recv, r_send, r_recv, z_send, z_recv,
    m_send, m_recv, l_send, l_recv, p_send, p_recv, oz_send, oz_recv, or_send, or_recv, og_send, og_recv, out_sem, blocks_sem,
):
    me, rep = lax.axis_index("obs"), lax.axis_index("rep")
    z, y, c, x = me // (NY * 2), lax.rem(me // 2, NY), lax.rem(me, 2), rep
    p = jnp.where(c == 0, x, y)
    q = jnp.where(c == 0, y, x)
    cap = jac.shape[1] // n
    width = part.shape[2]
    e = (x * NY + y) * 2 + c
    half, quarter = z // 4, lax.rem(z, 4)

    def at(zz, yy, cc, xx):
        return {"obs": (zz * NY + yy) * 2 + cc, "rep": xx}

    def cross(pp, qq):
        return at(z, jnp.where(c == 0, qq, pp), c, jnp.where(c == 0, pp, qq))

    chunks = load_sem.shape[0] - 3
    span = n // chunks
    loads = [pltpu.make_async_copy(s, d, load_sem.at[k]) for k, (s, d) in enumerate(((res_in, res), (ids_in, ids), (cmap_in, cmap)))]
    for k in range(chunks):
        lanes = pl.ds(k * span * cap, span * cap)
        loads.append(pltpu.make_async_copy(jac_in.at[:, lanes], jac.at[:, lanes], load_sem.at[3 + k]))
    for load in loads:
        load.start()
    barrier = pltpu.get_barrier_semaphore()

    def plane(i):
        ee = lax.rem(e + i, AGG)
        return at(z, lax.rem(ee // 2, NY), lax.rem(ee, 2), ee // (NY * 2))

    peers = [plane(i) for i in range(1, AGG)]
    for i in range(1, NZ):
        zz = lax.rem(z + i, NZ)
        peers.append(at(zz, y, c, x))
        peers.append(at(zz, y, 1 - c, x))
    for peer in peers:
        pl.semaphore_signal(barrier, inc=1, device_id=peer, device_id_type=MESH)
    part[...] = jnp.zeros_like(part)
    over[...] = jnp.zeros_like(over)
    spread[...] = jnp.zeros_like(spread)
    for load in loads:
        load.wait()
    place = lax.broadcasted_iota(jnp.int32, (1, LIVE), 1)

    def pack(ee, b):
        d = (ee // 8 * 2 + b) * 8 + lax.rem(ee, 8)
        lanes = pl.ds(pl.multiple_of(d * cap, cap), LIVE)
        packed[ee, b, 0:18, :] = jac[:, lanes]
        packed[ee, b, 18:20, :] = res[:, lanes]
        packed[ee, b, 20:21, :] = jnp.where(place < counts[0, d], ids[:, lanes], -1).astype(F32)

    def scan(d, carry):
        rest = pl.ds(pl.multiple_of(d * cap + LIVE, LIVE), LIVE)
        count = jnp.full((18, LIVE), counts[0, d], jnp.int32)
        late = jnp.where(place + LIVE < counts[0, d], ids[:, rest], -1).astype(F32)
        found = (jac[:, rest], res[:, rest], late, jnp.full((8, LIVE), d, jnp.int32))
        return tuple(jnp.where(count[0 : new.shape[0]] > LIVE, new, old) for new, old in zip(found, carry))

    kept = (jnp.zeros((18, LIVE), F32), jnp.zeros((2, LIVE), F32), jnp.full((1, LIVE), -1, F32), jnp.zeros((8, LIVE), jnp.int32))
    kept = lax.fori_loop(0, n, scan, kept, unroll=4)
    over_block[0:18, :] = kept[0]
    over_block[18:20, :] = kept[1]
    over_block[20:21, :] = kept[2]
    full[...] = kept[3]
    add_block(over_block[...], over)
    pl.semaphore_wait(barrier, len(peers))

    def remote(src, dst, s, r, peer):
        return pltpu.make_async_remote_copy(
            src_ref=src, dst_ref=dst, send_sem=s, recv_sem=r, device_id=peer, device_id_type=MESH
        )

    sent = []

    def send(*args):
        copy = remote(*args)
        copy.start()
        sent.append(copy)
        return copy

    def handing(k):
        i = AGG // 2 + (k + 1) // 2 * (1 - 2 * lax.rem(k, 2))
        return remote(packed.at[lax.rem(e + i, AGG)], moved.at[i], x_send.at[i], x_recv.at[i], plane(i))

    def start(k, carry):
        i = AGG // 2 + (k + 1) // 2 * (1 - 2 * lax.rem(k, 2))
        ee = lax.rem(e + i, AGG)
        pack(ee, 0)
        pack(ee, 1)
        handing(k).start()
        return carry

    def take(k, carry):
        i = AGG // 2 + (k + 1) // 2 * (1 - 2 * lax.rem(k, 2))
        handing(k).wait_recv()
        add_block(moved[i, 0], part.at[0:4])
        add_block(moved[i, 1], part.at[4:8])
        return carry

    def drain(k, carry):
        handing(k).wait_send()
        return carry

    far = (4, 3, 5, 2, 6, 1, 7)

    over_zs = []
    for i in far:
        zz = lax.rem(z + i, NZ)
        over_zs.append(send(over.at[lax.rem(zz, 4)], over_zin.at[i], oz_send.at[i], oz_recv.at[i], at(zz, y, c, x)))
    lax.fori_loop(0, AGG - 1, start, 0)
    pack(e, 0)
    pack(e, 1)
    add_block(packed[e, 0], part.at[0:4])
    add_block(packed[e, 1], part.at[4:8])

    def owner_lanes(a):
        owner = (a // NY * 2 + half) * 8 + lax.rem(a, NY) * 2 + c
        return pl.ds(pl.multiple_of(owner * CAM_DEV + quarter * width, width), width)

    def prepare(a, carry):
        ready[a] = one_hot_of(lax.rem(cmap[:, owner_lanes(a)], LOW), LOW)
        return carry

    lax.fori_loop(0, 16, prepare, 0)
    lax.fori_loop(0, 12, take, 0)
    for copy in over_zs:
        copy.wait_recv()
    mine = over[quarter]
    for i in range(1, NZ):
        mine = mine + over_zin[i]
    for k in range(ROWS // 2):
        over_s[k] = mine[k * 2 : k * 2 + 2]
    for k in range(ROWS // 2, AGG):
        over_s[k] = jnp.zeros_like(over_s[k])

    def scattering(i, carry):
        remote(over_s.at[lax.rem(e + i, AGG)], over_in.at[i], or_send.at[i], or_recv.at[i], plane(i)).start()
        return carry

    def gathering_over(i):
        slot = over_all.at[lax.rem(e + AGG - i, AGG)]
        return remote(slot, slot, og_send.at[i], og_recv.at[i], plane(i))

    def spreading(i, carry):
        slot = over_all.at[e]
        remote(slot, slot, og_send.at[i], og_recv.at[i], plane(i)).start()
        return carry

    def added(i, value):
        remote(over_s.at[i], over_in.at[i], or_send.at[i], or_recv.at[i], plane(i)).wait_recv()
        return value + over_in[i]

    def arrived(i, carry):
        gathering_over(i).wait_recv()
        return carry

    def drain_over(i, carry):
        remote(over_s.at[lax.rem(e + i, AGG)], over_in.at[i], or_send.at[i], or_recv.at[i], plane(i)).wait_send()
        gathering_over(i).wait_send()
        return carry

    lax.fori_loop(1, AGG, scattering, 0)
    lax.fori_loop(12, AGG - 1, take, 0)
    first, second = [], []
    for kind, rows, copies in ((0, pl.ds(0, HEAD), first), (1, pl.ds(HEAD, ROWS - HEAD), second)):
        for i in far:
            zz = lax.rem(z + i, NZ)
            copies.append(
                send(part.at[zz, rows], landed.at[i, rows], a_send.at[kind, i], a_recv.at[kind, i], at(zz, y, c, x))
            )
    over_all[e] = lax.fori_loop(1, AGG, added, over_s[e])
    lax.fori_loop(1, AGG, spreading, 0)
    lax.fori_loop(1, AGG, arrived, 0)
    bucket = (x * 2 + half) * 8 + y * 2 + c
    owned = full[...] == bucket
    for copy in first:
        copy.wait_recv()

    def total(g):
        rows = slice(g * 8, g * 8 + 8)
        value = part[z, rows] + jnp.where(owned, jnp.concatenate([over_all[g * 4 + i] for i in range(4)], axis=0), 0.0)
        for i in range(1, NZ):
            value = value + landed[i, rows]
        return value

    top, mix = total(0), total(1)
    a_me = x * NY + y
    gath[a_me, 0:8] = top[:, 0:128]
    gath[a_me, 8:16] = top[:, 128:256]
    gath[a_me, 16:17] = mix[5:6, 0:128]
    gath[a_me, 17:18] = mix[5:6, 128:256]
    def gathering(i):
        a, aa = lax.rem(a_me + 16 - i, 16), lax.rem(a_me + i, 16)
        return gath.at[a], at(z, lax.rem(aa, NY), c, aa // NY)

    for i in (8, 7, 9, 6, 10, 5, 11, 4, 12, 3, 13, 2, 14, 1, 15):
        send(gath.at[a_me], gath.at[a_me], g_send.at[i], g_recv.at[i], gathering(i)[1])
    row_blocks[x, 0:8] = mix
    def settle(i, carry):
        a = lax.rem(a_me + 16 - i, 16)
        place_source(gath[a], cmap[:, owner_lanes(a)] // LOW - a_me * 16, ready[a], spread)
        return carry

    def arrive(i, carry):
        slot, peer = gathering(i)
        remote(slot, slot, g_send.at[i], g_recv.at[i], peer).wait_recv()
        return settle(i, carry)

    settle(0, 0)
    lax.fori_loop(1, 16, arrive, 0)
    for u in range(16):
        value = spread[u * 16 : u * 16 + 8, :] + spread[u * 16 + 8 : u * 16 + 16, :]
        shares[u, 0:8] = value[:, 0:128]
        shares[u, 8:16] = value[:, 128:256]
        ninth = spread[256 + u : 257 + u, :] + spread[272 + u : 273 + u, :]
        shares[u, 16:17] = ninth[:, 0:128]
        shares[u, 17:18] = ninth[:, 128:256]
    s_me = z * 2 + c
    reduced = []
    for i in (8, 7, 9, 6, 10, 5, 11, 4, 12, 3, 13, 2, 14, 1, 15):
        ss = lax.rem(s_me + i, 16)
        reduced.append(send(shares.at[ss], got.at[i], r_send.at[i], r_recv.at[i], at(ss // 2, y, lax.rem(ss, 2), x)))
    for copy in second:
        copy.wait_recv()
    for g in range(2, 7):
        row_blocks[x, g * 8 - 8 : g * 8] = total(g)
    row = []
    for i in (1, 3, 2):
        piece = row_blocks.at[x]
        row.append(send(piece, piece, b_send.at[i], b_recv.at[i], at(z, y, c, lax.rem(x + i, NX))))
    for copy in reduced:
        copy.wait_recv()
    value = shares[s_me]
    for i in range(1, 16):
        value = value + got[i]
    every[c, p, q, z] = value[0:16]
    nine[c, p, q, z] = value[16:18]
    held = (every, nine)
    for i in far:
        for v in (0, 1):
            own = held[v].at[c, p, q, z]
            send(own, own, z_send.at[v, i], z_recv.at[v, i], at(lax.rem(z + i, NZ), y, c, x))
    for i in range(1, NZ):
        for v in (0, 1):
            slot = held[v].at[c, p, q, lax.rem(z + NZ - i, NZ)]
            remote(slot, slot, z_send.at[v, i], z_recv.at[v, i], at(lax.rem(z + i, NZ), y, c, x)).wait_recv()
    outs = []

    def put(v, cc, pp, qq):
        target = (all_out, nine_out)[v]
        copy = pltpu.make_async_copy(held[v].at[cc, pp, qq], target.at[cc, pp, qq], out_sem.at[v, cc, pp, qq])
        copy.start()
        outs.append(copy)

    other = at(z, y, 1 - c, x)

    def back(v, i):
        return lax.rem(v + 4 - i, 4)

    for i in (1, 3, 2):
        for v in (0, 1):
            group = held[v].at[c, p, q]
            send(group, group, m_send.at[v, i], m_recv.at[v, i], cross(p, lax.rem(q + i, 4)))
    for i in range(1, NX):
        piece = row_blocks.at[lax.rem(x + NX - i, NX)]
        remote(piece, piece, b_send.at[i], b_recv.at[i], at(z, y, c, lax.rem(x + i, NX))).wait_recv()

    def homing(k):
        return remote(row_blocks.at[k], blocks.at[quarter], h_send.at[k], h_recv.at[quarter], at(k * 2 + half, y, c, x))

    for k in range(NX):

        @pl.when(k * 2 + half != z)
        def _():
            homing(k).start()

        @pl.when(k * 2 + half == z)
        def _():
            blocks[quarter] = row_blocks[k]

    for i in (0, 1, 3, 2):
        for v in (0, 1):
            group = held[v].at[c, p, back(q, i)]
            if i:
                remote(group, group, m_send.at[v, i], m_recv.at[v, i], cross(p, lax.rem(q + i, 4))).wait_recv()
            for j in (1, 3, 2):
                send(group, group, l_send.at[v, j, i], l_recv.at[v, j, i], cross(lax.rem(p + j, 4), q))
            send(group, group, p_send.at[v, 0, i], p_recv.at[v, 0, i], other)
            put(v, c, p, back(q, i))
    for i in (0, 1, 3, 2):
        for j in (1, 3, 2):
            for v in (0, 1):
                group = held[v].at[c, back(p, j), back(q, i)]
                remote(group, group, l_send.at[v, j, i], l_recv.at[v, j, i], cross(lax.rem(p + j, 4), q)).wait_recv()
                send(group, group, p_send.at[v, j, i], p_recv.at[v, j, i], other)
                put(v, c, back(p, j), back(q, i))
    for k in range(4):
        slot = blocks.at[k]

        @pl.when(lax.rem(z, 2) * 4 + k != z)
        def _():
            remote(slot, slot, h_send.at[0], h_recv.at[k], at(lax.rem(z + 1, NZ), y, c, x)).wait_recv()

        @pl.when(k * 2 + half != z)
        def _():
            homing(k).wait_send()

    out_blocks = pltpu.make_async_copy(blocks, blocks_out, blocks_sem.at[0])
    out_blocks.start()
    for j in (0, 1, 3, 2):
        for i in (0, 1, 3, 2):
            for v in (0, 1):
                group = held[v].at[1 - c, back(q, j), back(p, i)]
                remote(group, group, p_send.at[v, j, i], p_recv.at[v, j, i], other).wait_recv()
                put(v, 1 - c, back(q, j), back(p, i))
    lax.fori_loop(0, AGG - 1, drain, 0)
    lax.fori_loop(1, AGG, drain_over, 0)
    for copy in sent:
        copy.wait_send()
    for copy in outs:
        copy.wait()
    out_blocks.wait()


def write_kernel(all_in, nine_in, blocks_in, gradient_out, blocks_out, held, nine, blocks, gradient, wide, in_sem, out_sem):
    last = NX * 2
    reads = [pltpu.make_async_copy(blocks_in, blocks, in_sem.at[0]), pltpu.make_async_copy(nine_in, nine, in_sem.at[1])]
    for k in range(last):
        x, some = k // 2, pl.ds(k % 2 * 2, 2)
        reads.append(pltpu.make_async_copy(all_in.at[0, x, some], held.at[0, x, some], in_sem.at[2 + k * 2]))
        reads.append(pltpu.make_async_copy(all_in.at[1, some, x], held.at[1, some, x], in_sem.at[3 + k * 2]))
    for read in reads:
        read.start()
    step = gradient.shape[1] // last
    writes = []

    def write(src, dst, k):
        copy = pltpu.make_async_copy(src, dst, out_sem.at[k])
        copy.start()
        writes.append(copy)

    reads[0].wait()
    pieces, _, width = blocks.shape
    for k in range(9):
        for l in range(9):
            row = block_row(k, l) - 8
            for r in range(pieces):
                wide[k * 9 + l : k * 9 + l + 1, r * width : (r + 1) * width] = blocks[r, row : row + 1, :]
    write(wide, blocks_out, last)
    reads[1].wait()
    for k in range(last):
        for read in reads[2 + k * 2 : 4 + k * 2]:
            read.wait()
        x = k // 2
        for block in range(32):
            y, z, c = k % 2 * 2 + block // 16, block // 2 % 8, block % 2
            p, q = (y, x) if c else (x, y)
            lanes = k * step + block * LOW
            gradient[0:8, lanes : lanes + 128] = held[c, p, q, z, 0:8]
            gradient[0:8, lanes + 128 : lanes + 256] = held[c, p, q, z, 8:16]
            gradient[8:9, lanes : lanes + 128] = nine[c, p, q, z, 0:1]
            gradient[8:9, lanes + 128 : lanes + 256] = nine[c, p, q, z, 1:2]
        lanes = pl.ds(k * step, step)
        write(gradient.at[:, lanes], gradient_out.at[:, lanes], k)
    for copy in writes:
        copy.wait()


def local(jacobians, residuals, camera_local, bucket_counts, camera_map):
    n, m = lax.axis_size("obs"), lax.axis_size("rep")
    slots = jacobians.shape[1]
    cams = camera_map.shape[0]
    width = CAM_DEV // m
    dma = pltpu.SemaphoreType.DMA
    limit = 60 * 1024 * 1024
    anywhere = pl.BlockSpec(memory_space=pl.ANY)
    hbm = pl.BlockSpec(memory_space=pltpu.HBM)
    gathered, ninth, blocks = pl.pallas_call(
        functools.partial(main_kernel, n, m),
        out_shape=(
            jax.ShapeDtypeStruct((2, 4, 4, NZ, 16, 128), F32),
            jax.ShapeDtypeStruct((2, 4, 4, NZ, 2, 128), F32),
            jax.ShapeDtypeStruct((m, KEPT, width), F32),
        ),
        in_specs=[pl.BlockSpec(memory_space=pltpu.SMEM)] + [hbm] * 4,
        out_specs=(hbm, hbm, hbm),
        scratch_shapes=[
            VMEM((18, slots), F32),
            VMEM((2, slots), F32),
            VMEM((1, slots), jnp.int32),
            VMEM((1, cams), jnp.int32),
            dma((3 + 4,)),
            VMEM((AGG, 2, 21, LIVE), F32),
            VMEM((AGG, 2, 21, LIVE), F32),
            VMEM((NZ, ROWS, width), F32),
            VMEM((NZ, ROWS, width), F32),
            VMEM((NX, KEPT, width), F32),
            VMEM((m, KEPT, width), F32),
            VMEM((16, 18, 128), F32),
            VMEM((16, LOW, width), BF16),
            VMEM((288, LOW), F32),
            VMEM((16, 18, 128), F32),
            VMEM((16, 18, 128), F32),
            VMEM((2, 4, 4, NZ, 16, 128), F32),
            VMEM((2, 4, 4, NZ, 2, 128), F32),
            VMEM((m, ROWS, width), F32),
            VMEM((21, LIVE), F32),
            VMEM((8, LIVE), jnp.int32),
            VMEM((NZ, ROWS, width), F32),
            VMEM((AGG, 2, width), F32),
            VMEM((AGG, 2, width), F32),
            VMEM((AGG, 2, width), F32),
        ]
        + [dma((AGG,))] * 2 + [dma((2, NZ))] * 2 + [dma((4,))] * 4 + [dma((16,))] * 4 + [dma((2, NZ))] * 2 + [dma((2, 4))] * 2
        + [dma((2, 4, 4))] * 4 + [dma((NZ,))] * 2 + [dma((AGG,))] * 4 + [dma((2, 2, 4, 4)), dma((1,))],
        compiler_params=pltpu.CompilerParams(collective_id=0, has_side_effects=True, vmem_limit_bytes=limit),
    )(bucket_counts, jacobians, residuals, camera_local.reshape(1, slots), camera_map.reshape(1, cams))
    shapes = (jax.ShapeDtypeStruct((9, cams), F32), jax.ShapeDtypeStruct((81, CAM_DEV), F32))
    return pl.pallas_call(
        write_kernel,
        out_shape=shapes,
        in_specs=[anywhere] * 3,
        out_specs=(anywhere, anywhere),
        scratch_shapes=[
            VMEM(gathered.shape, F32), VMEM(ninth.shape, F32), VMEM(blocks.shape, F32), VMEM(shapes[0].shape, F32),
            VMEM(shapes[1].shape, F32), dma((NX * 4 + 2,)), dma((NX * 2 + 1,)),
        ],
        compiler_params=pltpu.CompilerParams(vmem_limit_bytes=limit),
    )(gathered, ninth, blocks)


def solution(mesh):
    in_specs = (
        P(None, ("obs", "rep")),
        P(None, ("obs", "rep")),
        P(("obs", "rep")),
        P(("obs", "rep"), None),
        P(),
    )
    out_specs = (P(), P(None, "obs"))
    return jax.shard_map(local, mesh=mesh, in_specs=in_specs, out_specs=out_specs, check_vma=False)
```

```python
import functools

import jax
import jax.numpy as jnp
from jax import lax
from jax.experimental import pallas as pl
from jax.experimental.pallas import tpu as pltpu
from jax.sharding import PartitionSpec as P

CAM_DEV = 1024
MESH = pl.DeviceIdType.MESH
F32 = jnp.float32
BF16 = jnp.bfloat16
VMEM = pltpu.VMEM
ROWS = 56
HEAD = 16
KEPT = 48
LOW = 256
LIVE = 256
NZ, NY, NX = 8, 4, 4
AGG = NX * NY * 2
DIMS = (((1,), (1,)), ((), ()))


def split(value):
    high = value.astype(BF16).astype(F32)
    return high, value - high


def one_hot_of(low, wide):
    shape = (wide, low.shape[1])
    rows = lax.broadcasted_iota(jnp.int32, shape, 0).astype(F32).astype(BF16)
    there = jnp.broadcast_to(low.astype(F32), shape).astype(BF16)
    return jnp.where(there == rows, jnp.ones(shape, BF16), jnp.zeros(shape, BF16))


def turn(value, j):
    return jnp.concatenate([value[j:8], value[0:j]], axis=0)


def block_row(k, l):
    k, l = min(k, l), max(k, l)
    if l == 8:
        return 12 if k == 8 else 48 + k
    j = l - k
    if j < 4:
        return 16 + 8 * j + k
    if j == 4:
        return 8 + k
    return 16 + 8 * (8 - j) + l


def add_block(block, acc):
    lead, trail = block[0:8], block[9:17]
    lead8, trail8, res0, res1 = block[8:9], block[17:18], block[18:19], block[19:20]
    ids = block[20:21].astype(jnp.int32)
    place = lax.broadcasted_iota(jnp.int32, lead.shape, 0)

    def mixed(rows, ninth, res):
        left = jnp.where(place < 4, rows, ninth)
        right = jnp.where(place < 4, turn(rows, 4), jnp.where(place == 4, ninth, res))
        return left * right

    groups = [lead * res0 + trail * res1, mixed(lead, lead8, res0) + mixed(trail, trail8, res1)]
    groups.append(lead * lead + trail * trail)
    for j in range(1, 4):
        groups.append(lead * turn(lead, j) + trail * turn(trail, j))
    groups.append(lead * lead8 + trail * trail8)
    high, low = split(jnp.concatenate(groups, axis=0))
    both = jnp.concatenate([high, low], axis=0).astype(BF16)
    pieces, _, width = acc.shape
    up = jnp.where(ids < 0, -1, ids // width)
    one_hot = one_hot_of(ids - up * width, width)
    up = jnp.broadcast_to(up.astype(F32), both.shape).astype(BF16)
    zero = jnp.zeros_like(both)
    lhs = jnp.concatenate([jnp.where(up == jnp.asarray(h, BF16), both, zero) for h in range(pieces)], axis=0)
    added = lax.dot_general(lhs, one_hot, DIMS, preferred_element_type=F32)
    for h in range(pieces):
        at = h * 2 * ROWS
        acc[h, 0:ROWS] += added[at : at + ROWS] + added[at + ROWS : at + 2 * ROWS]


def place_source(block, up, one_hot, acc):
    rows = jnp.concatenate([block[0:8], block[8:16]], axis=1)
    ninth = jnp.concatenate([block[16:17], block[17:18]], axis=1)
    high, low = split(rows)
    top = jnp.concatenate([high, low], axis=0).astype(BF16)
    high9, low9 = split(ninth)
    up16 = jnp.broadcast_to(up.astype(F32), top.shape).astype(BF16)
    none = jnp.zeros_like(top)
    tiles = [jnp.where(up16 == jnp.asarray(h, BF16), top, none) for h in range(16)]
    mask = up == lax.broadcasted_iota(jnp.int32, (16, up.shape[1]), 0)
    tiles.append(jnp.where(mask, high9, 0.0).astype(BF16))
    tiles.append(jnp.where(mask, low9, 0.0).astype(BF16))
    acc[...] += lax.dot_general(jnp.concatenate(tiles, axis=0), one_hot, DIMS, preferred_element_type=F32)


def main_kernel(
    n, m, counts, jac_in, res_in, ids_in, cmap_in, all_out, nine_out, blocks_out,
    jac, res, ids, cmap, load_sem, packed, moved, part, landed, row_blocks, blocks, gath, ready, spread, shares, got,
    every, nine, over, over_block, full, over_zin, over_s, over_in, over_all,
    x_send, x_recv, a_send, a_recv, b_send, b_recv, h_send, h_recv, g_send, g_recv, r_send, r_recv, z_send, z_recv,
    m_send, m_recv, l_send, l_recv, p_send, p_recv, oz_send, oz_recv, or_send, or_recv, og_send, og_recv, out_sem, blocks_sem,
):
    me, rep = lax.axis_index("obs"), lax.axis_index("rep")
    z, y, c, x = me // (NY * 2), lax.rem(me // 2, NY), lax.rem(me, 2), rep
    p = jnp.where(c == 0, x, y)
    q = jnp.where(c == 0, y, x)
    cap = jac.shape[1] // n
    width = part.shape[2]
    e = (x * NY + y) * 2 + c
    half, quarter = z // 4, lax.rem(z, 4)

    def at(zz, yy, cc, xx):
        return {"obs": (zz * NY + yy) * 2 + cc, "rep": xx}

    def cross(pp, qq):
        return at(z, jnp.where(c == 0, qq, pp), c, jnp.where(c == 0, pp, qq))

    chunks = load_sem.shape[0] - 3
    span = n // chunks
    loads = [pltpu.make_async_copy(s, d, load_sem.at[k]) for k, (s, d) in enumerate(((res_in, res), (ids_in, ids), (cmap_in, cmap)))]
    for k in range(chunks):
        lanes = pl.ds(k * span * cap, span * cap)
        loads.append(pltpu.make_async_copy(jac_in.at[:, lanes], jac.at[:, lanes], load_sem.at[3 + k]))
    for load in loads:
        load.start()
    barrier = pltpu.get_barrier_semaphore()

    def plane(i):
        ee = lax.rem(e + i, AGG)
        return at(z, lax.rem(ee // 2, NY), lax.rem(ee, 2), ee // (NY * 2))

    peers = [plane(i) for i in range(1, AGG)]
    for i in range(1, NZ):
        zz = lax.rem(z + i, NZ)
        peers.append(at(zz, y, c, x))
        peers.append(at(zz, y, 1 - c, x))
    for peer in peers:
        pl.semaphore_signal(barrier, inc=1, device_id=peer, device_id_type=MESH)
    part[...] = jnp.zeros_like(part)
    over[...] = jnp.zeros_like(over)
    spread[...] = jnp.zeros_like(spread)
    for load in loads:
        load.wait()
    place = lax.broadcasted_iota(jnp.int32, (1, LIVE), 1)

    def pack(ee, b):
        d = (ee // 8 * 2 + b) * 8 + lax.rem(ee, 8)
        lanes = pl.ds(pl.multiple_of(d * cap, cap), LIVE)
        packed[ee, b, 0:18, :] = jac[:, lanes]
        packed[ee, b, 18:20, :] = res[:, lanes]
        packed[ee, b, 20:21, :] = jnp.where(place < counts[0, d], ids[:, lanes], -1).astype(F32)

    def scan(d, carry):
        rest = pl.ds(pl.multiple_of(d * cap + LIVE, LIVE), LIVE)
        count = jnp.full((18, LIVE), counts[0, d], jnp.int32)
        late = jnp.where(place + LIVE < counts[0, d], ids[:, rest], -1).astype(F32)
        found = (jac[:, rest], res[:, rest], late, jnp.full((8, LIVE), d, jnp.int32))
        return tuple(jnp.where(count[0 : new.shape[0]] > LIVE, new, old) for new, old in zip(found, carry))

    kept = (jnp.zeros((18, LIVE), F32), jnp.zeros((2, LIVE), F32), jnp.full((1, LIVE), -1, F32), jnp.zeros((8, LIVE), jnp.int32))
    kept = lax.fori_loop(0, n, scan, kept, unroll=4)
    over_block[0:18, :] = kept[0]
    over_block[18:20, :] = kept[1]
    over_block[20:21, :] = kept[2]
    full[...] = kept[3]
    add_block(over_block[...], over)
    pl.semaphore_wait(barrier, len(peers))

    def remote(src, dst, s, r, peer):
        return pltpu.make_async_remote_copy(
            src_ref=src, dst_ref=dst, send_sem=s, recv_sem=r, device_id=peer, device_id_type=MESH
        )

    sent = []

    def send(*args):
        copy = remote(*args)
        copy.start()
        sent.append(copy)
        return copy

    def handing(k):
        i = AGG // 2 + (k + 1) // 2 * (1 - 2 * lax.rem(k, 2))
        return remote(packed.at[lax.rem(e + i, AGG)], moved.at[i], x_send.at[i], x_recv.at[i], plane(i))

    def start(k, carry):
        i = AGG // 2 + (k + 1) // 2 * (1 - 2 * lax.rem(k, 2))
        ee = lax.rem(e + i, AGG)
        pack(ee, 0)
        pack(ee, 1)
        handing(k).start()
        return carry

    def take(k, carry):
        i = AGG // 2 + (k + 1) // 2 * (1 - 2 * lax.rem(k, 2))
        handing(k).wait_recv()
        add_block(moved[i, 0], part.at[0:4])
        add_block(moved[i, 1], part.at[4:8])
        return carry

    def drain(k, carry):
        handing(k).wait_send()
        return carry

    far = (4, 3, 5, 2, 6, 1, 7)

    over_zs = []
    for i in far:
        zz = lax.rem(z + i, NZ)
        over_zs.append(send(over.at[lax.rem(zz, 4)], over_zin.at[i], oz_send.at[i], oz_recv.at[i], at(zz, y, c, x)))
    lax.fori_loop(0, AGG - 1, start, 0)
    pack(e, 0)
    pack(e, 1)
    add_block(packed[e, 0], part.at[0:4])
    add_block(packed[e, 1], part.at[4:8])

    def owner_lanes(a):
        owner = (a // NY * 2 + half) * 8 + lax.rem(a, NY) * 2 + c
        return pl.ds(pl.multiple_of(owner * CAM_DEV + quarter * width, width), width)

    def prepare(a, carry):
        ready[a] = one_hot_of(lax.rem(cmap[:, owner_lanes(a)], LOW), LOW)
        return carry

    lax.fori_loop(0, 16, prepare, 0)
    lax.fori_loop(0, 10, take, 0)
    for copy in over_zs:
        copy.wait_recv()
    mine = over[quarter]
    for i in range(1, NZ):
        mine = mine + over_zin[i]
    for k in range(ROWS // 2):
        over_s[k] = mine[k * 2 : k * 2 + 2]
    for k in range(ROWS // 2, AGG):
        over_s[k] = jnp.zeros_like(over_s[k])

    def scattering(i, carry):
        remote(over_s.at[lax.rem(e + i, AGG)], over_in.at[i], or_send.at[i], or_recv.at[i], plane(i)).start()
        return carry

    def gathering_over(i):
        slot = over_all.at[lax.rem(e + AGG - i, AGG)]
        return remote(slot, slot, og_send.at[i], og_recv.at[i], plane(i))

    def spreading(i, carry):
        slot = over_all.at[e]
        remote(slot, slot, og_send.at[i], og_recv.at[i], plane(i)).start()
        return carry

    def added(i, value):
        remote(over_s.at[i], over_in.at[i], or_send.at[i], or_recv.at[i], plane(i)).wait_recv()
        return value + over_in[i]

    def arrived(i, carry):
        gathering_over(i).wait_recv()
        return carry

    def drain_over(i, carry):
        remote(over_s.at[lax.rem(e + i, AGG)], over_in.at[i], or_send.at[i], or_recv.at[i], plane(i)).wait_send()
        gathering_over(i).wait_send()
        return carry

    lax.fori_loop(1, AGG, scattering, 0)
    lax.fori_loop(10, AGG - 1, take, 0)
    first, second = [], []
    for kind, rows, copies in ((0, pl.ds(0, HEAD), first), (1, pl.ds(HEAD, ROWS - HEAD), second)):
        for i in far:
            zz = lax.rem(z + i, NZ)
            copies.append(
                send(part.at[zz, rows], landed.at[i, rows], a_send.at[kind, i], a_recv.at[kind, i], at(zz, y, c, x))
            )
    over_all[e] = lax.fori_loop(1, AGG, added, over_s[e])
    lax.fori_loop(1, AGG, spreading, 0)
    lax.fori_loop(1, AGG, arrived, 0)
    bucket = (x * 2 + half) * 8 + y * 2 + c
    owned = full[...] == bucket
    for copy in first:
        copy.wait_recv()

    def total(g):
        rows = slice(g * 8, g * 8 + 8)
        value = part[z, rows] + jnp.where(owned, jnp.concatenate([over_all[g * 4 + i] for i in range(4)], axis=0), 0.0)
        for i in range(1, NZ):
            value = value + landed[i, rows]
        return value

    top, mix = total(0), total(1)
    a_me = x * NY + y
    gath[a_me, 0:8] = top[:, 0:128]
    gath[a_me, 8:16] = top[:, 128:256]
    gath[a_me, 16:17] = mix[5:6, 0:128]
    gath[a_me, 17:18] = mix[5:6, 128:256]
    def gathering(i):
        a, aa = lax.rem(a_me + 16 - i, 16), lax.rem(a_me + i, 16)
        return gath.at[a], at(z, lax.rem(aa, NY), c, aa // NY)

    for i in (8, 7, 9, 6, 10, 5, 11, 4, 12, 3, 13, 2, 14, 1, 15):
        send(gath.at[a_me], gath.at[a_me], g_send.at[i], g_recv.at[i], gathering(i)[1])
    row_blocks[x, 0:8] = mix
    def settle(i, carry):
        a = lax.rem(a_me + 16 - i, 16)
        place_source(gath[a], cmap[:, owner_lanes(a)] // LOW - a_me * 16, ready[a], spread)
        return carry

    def arrive(i, carry):
        slot, peer = gathering(i)
        remote(slot, slot, g_send.at[i], g_recv.at[i], peer).wait_recv()
        return settle(i, carry)

    settle(0, 0)
    lax.fori_loop(1, 16, arrive, 0)
    for u in range(16):
        value = spread[u * 16 : u * 16 + 8, :] + spread[u * 16 + 8 : u * 16 + 16, :]
        shares[u, 0:8] = value[:, 0:128]
        shares[u, 8:16] = value[:, 128:256]
        ninth = spread[256 + u : 257 + u, :] + spread[272 + u : 273 + u, :]
        shares[u, 16:17] = ninth[:, 0:128]
        shares[u, 17:18] = ninth[:, 128:256]
    s_me = z * 2 + c
    reduced = []
    for i in (8, 7, 9, 6, 10, 5, 11, 4, 12, 3, 13, 2, 14, 1, 15):
        ss = lax.rem(s_me + i, 16)
        reduced.append(send(shares.at[ss], got.at[i], r_send.at[i], r_recv.at[i], at(ss // 2, y, lax.rem(ss, 2), x)))
    for copy in second:
        copy.wait_recv()
    for g in range(2, 7):
        row_blocks[x, g * 8 - 8 : g * 8] = total(g)
    row = []
    for i in (1, 3, 2):
        piece = row_blocks.at[x]
        row.append(send(piece, piece, b_send.at[i], b_recv.at[i], at(z, y, c, lax.rem(x + i, NX))))
    for copy in reduced:
        copy.wait_recv()
    value = shares[s_me]
    for i in range(1, 16):
        value = value + got[i]
    every[c, p, q, z] = value[0:16]
    nine[c, p, q, z] = value[16:18]
    held = (every, nine)
    for i in far:
        for v in (0, 1):
            own = held[v].at[c, p, q, z]
            send(own, own, z_send.at[v, i], z_recv.at[v, i], at(lax.rem(z + i, NZ), y, c, x))
    def onward(v, src):
        for i in (1, 3, 2):
            remote(src, src, m_send.at[v, i], m_recv.at[v, i], cross(p, lax.rem(q + i, 4))).start()
            remote(src, src, l_send.at[v, i, 0], l_recv.at[v, i, 0], cross(lax.rem(p + i, 4), q)).start()

    onward(0, every.at[c, p, q, z])
    for i in (1, 7, 2, 6, 3, 5, 4):
        for v in (0, 1):
            slot = held[v].at[c, p, q, lax.rem(z + NZ - i, NZ)]
            remote(slot, slot, z_send.at[v, i], z_recv.at[v, i], at(lax.rem(z + i, NZ), y, c, x)).wait_recv()
            if v == 0:
                onward(0, slot)
    onward(1, nine.at[c, p, q])
    outs = []

    def put(v, cc, pp, qq):
        target = (all_out, nine_out)[v]
        copy = pltpu.make_async_copy(held[v].at[cc, pp, qq], target.at[cc, pp, qq], out_sem.at[v, cc, pp, qq])
        copy.start()
        outs.append(copy)

    other = at(z, y, 1 - c, x)

    def back(v, i):
        return lax.rem(v + 4 - i, 4)

    for i in range(1, NX):
        piece = row_blocks.at[lax.rem(x + NX - i, NX)]
        remote(piece, piece, b_send.at[i], b_recv.at[i], at(z, y, c, lax.rem(x + i, NX))).wait_recv()

    def homing(k):
        return remote(row_blocks.at[k], blocks.at[quarter], h_send.at[k], h_recv.at[quarter], at(k * 2 + half, y, c, x))

    for k in range(NX):

        @pl.when(k * 2 + half != z)
        def _():
            homing(k).start()

        @pl.when(k * 2 + half == z)
        def _():
            blocks[quarter] = row_blocks[k]

    for i in (0, 1, 3, 2):
        for v in (0, 1):
            group = held[v].at[c, p, back(q, i)]
            if i:
                remote(group, group, m_send.at[v, i], m_recv.at[v, i], cross(p, lax.rem(q + i, 4))).wait_recv()
            if i:
                for j in (1, 3, 2):
                    send(group, group, l_send.at[v, j, i], l_recv.at[v, j, i], cross(lax.rem(p + j, 4), q))
            send(group, group, p_send.at[v, 0, i], p_recv.at[v, 0, i], other)
            put(v, c, p, back(q, i))
    for i in (0, 1, 3, 2):
        for j in (1, 3, 2):
            for v in (0, 1):
                group = held[v].at[c, back(p, j), back(q, i)]
                remote(group, group, l_send.at[v, j, i], l_recv.at[v, j, i], cross(lax.rem(p + j, 4), q)).wait_recv()
                send(group, group, p_send.at[v, j, i], p_recv.at[v, j, i], other)
                put(v, c, back(p, j), back(q, i))
    for k in range(4):
        slot = blocks.at[k]

        @pl.when(lax.rem(z, 2) * 4 + k != z)
        def _():
            remote(slot, slot, h_send.at[0], h_recv.at[k], at(lax.rem(z + 1, NZ), y, c, x)).wait_recv()

        @pl.when(k * 2 + half != z)
        def _():
            homing(k).wait_send()

    out_blocks = pltpu.make_async_copy(blocks, blocks_out, blocks_sem.at[0])
    out_blocks.start()
    for j in (0, 1, 3, 2):
        for i in (0, 1, 3, 2):
            for v in (0, 1):
                group = held[v].at[1 - c, back(q, j), back(p, i)]
                remote(group, group, p_send.at[v, j, i], p_recv.at[v, j, i], other).wait_recv()
                put(v, 1 - c, back(q, j), back(p, i))
    for v in (0, 1):
        group = held[v].at[c, p, q]
        for i in (1, 3, 2):
            remote(group, group, m_send.at[v, i], m_recv.at[v, i], cross(p, lax.rem(q + i, 4))).wait_send()
            remote(group, group, l_send.at[v, i, 0], l_recv.at[v, i, 0], cross(lax.rem(p + i, 4), q)).wait_send()
    lax.fori_loop(0, AGG - 1, drain, 0)
    lax.fori_loop(1, AGG, drain_over, 0)
    for copy in sent:
        copy.wait_send()
    for copy in outs:
        copy.wait()
    out_blocks.wait()


def write_kernel(all_in, nine_in, blocks_in, gradient_out, blocks_out, held, nine, blocks, gradient, wide, in_sem, out_sem):
    last = NX * 2
    reads = [pltpu.make_async_copy(blocks_in, blocks, in_sem.at[0]), pltpu.make_async_copy(nine_in, nine, in_sem.at[1])]
    for k in range(last):
        x, some = k // 2, pl.ds(k % 2 * 2, 2)
        reads.append(pltpu.make_async_copy(all_in.at[0, x, some], held.at[0, x, some], in_sem.at[2 + k * 2]))
        reads.append(pltpu.make_async_copy(all_in.at[1, some, x], held.at[1, some, x], in_sem.at[3 + k * 2]))
    for read in reads:
        read.start()
    step = gradient.shape[1] // last
    writes = []

    def write(src, dst, k):
        copy = pltpu.make_async_copy(src, dst, out_sem.at[k])
        copy.start()
        writes.append(copy)

    reads[0].wait()
    pieces, _, width = blocks.shape
    for k in range(9):
        for l in range(9):
            row = block_row(k, l) - 8
            for r in range(pieces):
                wide[k * 9 + l : k * 9 + l + 1, r * width : (r + 1) * width] = blocks[r, row : row + 1, :]
    write(wide, blocks_out, last)
    reads[1].wait()
    for k in range(last):
        for read in reads[2 + k * 2 : 4 + k * 2]:
            read.wait()
        x = k // 2
        for block in range(32):
            y, z, c = k % 2 * 2 + block // 16, block // 2 % 8, block % 2
            p, q = (y, x) if c else (x, y)
            lanes = k * step + block * LOW
            gradient[0:8, lanes : lanes + 128] = held[c, p, q, z, 0:8]
            gradient[0:8, lanes + 128 : lanes + 256] = held[c, p, q, z, 8:16]
            gradient[8:9, lanes : lanes + 128] = nine[c, p, q, z, 0:1]
            gradient[8:9, lanes + 128 : lanes + 256] = nine[c, p, q, z, 1:2]
        lanes = pl.ds(k * step, step)
        write(gradient.at[:, lanes], gradient_out.at[:, lanes], k)
    for copy in writes:
        copy.wait()


def local(jacobians, residuals, camera_local, bucket_counts, camera_map):
    n, m = lax.axis_size("obs"), lax.axis_size("rep")
    slots = jacobians.shape[1]
    cams = camera_map.shape[0]
    width = CAM_DEV // m
    dma = pltpu.SemaphoreType.DMA
    limit = 60 * 1024 * 1024
    anywhere = pl.BlockSpec(memory_space=pl.ANY)
    hbm = pl.BlockSpec(memory_space=pltpu.HBM)
    gathered, ninth, blocks = pl.pallas_call(
        functools.partial(main_kernel, n, m),
        out_shape=(
            jax.ShapeDtypeStruct((2, 4, 4, NZ, 16, 128), F32),
            jax.ShapeDtypeStruct((2, 4, 4, NZ, 2, 128), F32),
            jax.ShapeDtypeStruct((m, KEPT, width), F32),
        ),
        in_specs=[pl.BlockSpec(memory_space=pltpu.SMEM)] + [hbm] * 4,
        out_specs=(hbm, hbm, hbm),
        scratch_shapes=[
            VMEM((18, slots), F32),
            VMEM((2, slots), F32),
            VMEM((1, slots), jnp.int32),
            VMEM((1, cams), jnp.int32),
            dma((3 + 4,)),
            VMEM((AGG, 2, 21, LIVE), F32),
            VMEM((AGG, 2, 21, LIVE), F32),
            VMEM((NZ, ROWS, width), F32),
            VMEM((NZ, ROWS, width), F32),
            VMEM((NX, KEPT, width), F32),
            VMEM((m, KEPT, width), F32),
            VMEM((16, 18, 128), F32),
            VMEM((16, LOW, width), BF16),
            VMEM((288, LOW), F32),
            VMEM((16, 18, 128), F32),
            VMEM((16, 18, 128), F32),
            VMEM((2, 4, 4, NZ, 16, 128), F32),
            VMEM((2, 4, 4, NZ, 2, 128), F32),
            VMEM((m, ROWS, width), F32),
            VMEM((21, LIVE), F32),
            VMEM((8, LIVE), jnp.int32),
            VMEM((NZ, ROWS, width), F32),
            VMEM((AGG, 2, width), F32),
            VMEM((AGG, 2, width), F32),
            VMEM((AGG, 2, width), F32),
        ]
        + [dma((AGG,))] * 2 + [dma((2, NZ))] * 2 + [dma((4,))] * 4 + [dma((16,))] * 4 + [dma((2, NZ))] * 2 + [dma((2, 4))] * 2
        + [dma((2, 4, 4))] * 4 + [dma((NZ,))] * 2 + [dma((AGG,))] * 4 + [dma((2, 2, 4, 4)), dma((1,))],
        compiler_params=pltpu.CompilerParams(collective_id=0, has_side_effects=True, vmem_limit_bytes=limit),
    )(bucket_counts, jacobians, residuals, camera_local.reshape(1, slots), camera_map.reshape(1, cams))
    shapes = (jax.ShapeDtypeStruct((9, cams), F32), jax.ShapeDtypeStruct((81, CAM_DEV), F32))
    return pl.pallas_call(
        write_kernel,
        out_shape=shapes,
        in_specs=[anywhere] * 3,
        out_specs=(anywhere, anywhere),
        scratch_shapes=[
            VMEM(gathered.shape, F32), VMEM(ninth.shape, F32), VMEM(blocks.shape, F32), VMEM(shapes[0].shape, F32),
            VMEM(shapes[1].shape, F32), dma((NX * 4 + 2,)), dma((NX * 2 + 1,)),
        ],
        compiler_params=pltpu.CompilerParams(vmem_limit_bytes=limit),
    )(gathered, ninth, blocks)


def solution(mesh):
    in_specs = (
        P(None, ("obs", "rep")),
        P(None, ("obs", "rep")),
        P(("obs", "rep")),
        P(("obs", "rep"), None),
        P(),
    )
    out_specs = (P(), P(None, "obs"))
    return jax.shard_map(local, mesh=mesh, in_specs=in_specs, out_specs=out_specs, check_vma=False)
```
